128 devices in a mesh: mpo: 4 (over z), col: 4 (over y), row: 8 (over x, core).
Axes of the slice: x: 4, y: 4, z: 4, core: 2. Of those that a mesh axis runs over, the one named last changes fastest.
Arguments:
- psi_init: float32 [2048, 2, 2, 2048], P('row', None, None, 'col')
- left_env: float32 [2048, 8, 2048], P('row', 'mpo')
- right_env: float32 [2048, 8, 2048], P('col', 'mpo')
- mpo_w12: float32 [8, 8, 2, 2, 2, 2], P('mpo')
Outputs:
- output 1: float32 [4], replicated
- output 2: float32 [4], replicated
- output 3: float32 [2048, 2, 2, 2048], P('row', None, None, 'col')
All inputs are finite; a program needn't handle non-finite values.
Results may differ from the reference program's by a relative error of at most 0.001.
Values sent between devices are 32-bit elements.
A program may use at most 1 GiB of HBM per device.

```python
import jax
import jax.numpy as jnp
from jax import lax

BOND_DIM = 2048
PHYS_DIM = 2
MPO_BOND = 8
LANCZOS_STEPS = 4

PHYS_SQ = PHYS_DIM * PHYS_DIM
ROW_BLOCK = min(BOND_DIM, 32)
PREC_HIGH = lax.Precision.HIGHEST


def setup_inputs(seed: int = 0) -> dict:
    root_key = jax.random.key(seed)
    sub_keys = jax.random.split(root_key, 7)
    psi_init = jax.random.normal(sub_keys[0], (BOND_DIM, PHYS_DIM, PHYS_DIM, BOND_DIM), jnp.float32)
    eye_bond = jnp.eye(BOND_DIM, dtype=jnp.float32)
    g_left = jax.random.normal(sub_keys[1], (BOND_DIM, MPO_BOND, BOND_DIM), jnp.float32)
    c_left = jax.random.uniform(sub_keys[2], (MPO_BOND,), jnp.float32, 0.5, 1.5)
    left_env = (g_left + jnp.transpose(g_left, (2, 1, 0))) * (0.5 / BOND_DIM ** 0.5) + eye_bond[:, None, :] * c_left[None, :, None]
    g_right = jax.random.normal(sub_keys[3], (BOND_DIM, MPO_BOND, BOND_DIM), jnp.float32)
    c_right = jax.random.uniform(sub_keys[4], (MPO_BOND,), jnp.float32, 0.5, 1.5)
    right_env = (g_right + jnp.transpose(g_right, (2, 1, 0))) * (0.5 / BOND_DIM ** 0.5) + eye_bond[:, None, :] * c_right[None, :, None]
    w_noise = jax.random.normal(sub_keys[5], (MPO_BOND, MPO_BOND, PHYS_SQ, PHYS_SQ), jnp.float32)
    w_noise = (w_noise + jnp.transpose(w_noise, (0, 1, 3, 2))) * (0.5 ** 0.5 / (MPO_BOND * PHYS_DIM))
    w_diag = (2.0 + MPO_BOND * jax.random.normal(sub_keys[6], (MPO_BOND, MPO_BOND), jnp.float32)) / (MPO_BOND * MPO_BOND)
    mpo_w12 = (w_noise + w_diag[:, :, None, None] * jnp.eye(PHYS_SQ, dtype=jnp.float32)).reshape(MPO_BOND, MPO_BOND, PHYS_DIM, PHYS_DIM, PHYS_DIM, PHYS_DIM)
    return {'psi_init': psi_init, 'left_env': left_env, 'right_env': right_env, 'mpo_w12': mpo_w12}


def apply_ham(vec_in, left_env, right_env, mpo_w12):
    vec_mat = vec_in.reshape(BOND_DIM, PHYS_SQ, BOND_DIM)
    mpo_mat = mpo_w12.reshape(MPO_BOND, MPO_BOND, PHYS_SQ, PHYS_SQ)
    n_blocks = BOND_DIM // ROW_BLOCK
    left_blocks = jnp.transpose(left_env.reshape(BOND_DIM, MPO_BOND, n_blocks, ROW_BLOCK), (2, 0, 1, 3))

    def one_block(left_blk):
        t_one = jnp.einsum('alc,asb->lcsb', left_blk, vec_mat, precision=PREC_HIGH)
        t_two = jnp.einsum('lcsb,lrst->cbrt', t_one, mpo_mat, precision=PREC_HIGH)
        return jnp.einsum('cbrt,brd->ctd', t_two, right_env, precision=PREC_HIGH)

    out_blocks = lax.map(one_block, left_blocks)
    return out_blocks.reshape(BOND_DIM, PHYS_DIM, PHYS_DIM, BOND_DIM)


def reference(psi_init, left_env, right_env, mpo_w12):
    vec_cur = psi_init / jnp.sqrt(jnp.sum(psi_init * psi_init))
    vec_prev = jnp.zeros_like(vec_cur)
    beta_prev = jnp.zeros((), jnp.float32)
    alpha_list = []
    beta_list = []
    for step_idx in range(LANCZOS_STEPS):
        h_vec = apply_ham(vec_cur, left_env, right_env, mpo_w12)
        alpha_j = jnp.sum(vec_cur * h_vec)
        residual = h_vec - alpha_j * vec_cur - beta_prev * vec_prev
        beta_j = jnp.sqrt(jnp.sum(residual * residual))
        vec_prev = vec_cur
        vec_cur = residual / beta_j
        beta_prev = beta_j
        alpha_list.append(alpha_j)
        beta_list.append(beta_j)
    return jnp.stack(alpha_list), jnp.stack(beta_list), vec_cur
```

```python
import jax
import jax.numpy as jnp
from jax import lax
from jax.experimental import pallas as pl
from jax.experimental.pallas import tpu as pltpu
from jax.sharding import PartitionSpec as P

STEPS = 4
F32 = jnp.float32
MIB = 2**20


(FAR_P, FAR_M, NEAR_P, NEAR_M, LO, HI, OWN_P, OWN_M, OWN_D, ALT_P, ALT_M, ALT_D, FWD_P, DP_O, DM_O, DP_A, DM_A,
 FWD_M, DF_O, DF_A) = range(20)
N_COPY, N_REDUCE = 20, 5


HALVES = (0, 1)
OTHERS = (1, 2, 3)
FAR_FIRST = (2, 1, 3)
CHIPS, CORES, ROWS = 4, 2, 8


def dot_hi(a, b):
    return lax.dot_general(a, b, (((1,), (0,)), ((), ())), precision=lax.Precision.HIGHEST, preferred_element_type=F32)


def hi_of(z):
    return lax.div(z, 2)


def lo_of(z):
    return lax.rem(lax.div(z + 1, 2), 2)


def remote(src, dst, send, recv, device):
    return pltpu.make_async_remote_copy(src_ref=src, dst_ref=dst, send_sem=send, recv_sem=recv, device_id=device,
                                        device_id_type=pl.DeviceIdType.MESH)


def signal(sem, device):
    pl.semaphore_signal(sem, inc=1, device_id=device, device_id_type=pl.DeviceIdType.MESH)


def block(start, n):
    return pl.ds(pl.multiple_of(start, n), n)


class Around:
    def __init__(self):
        self.row, self.col, self.mpo = (lax.axis_index(a) for a in ('row', 'col', 'mpo'))
        self.x, self.c = lax.div(self.row, CORES), lax.rem(self.row, CORES)
        self.hi, self.lo = hi_of(self.mpo), lo_of(self.mpo)
        (self.xp, self.x2, self.xm), (self.yp, self.y2, self.ym) = (
            [lax.rem(v + d, CHIPS) for d in OTHERS] for v in (self.x, self.col))
        self.other = 1 - self.c
        self.to_xp, self.to_xm = ({'row': v * CORES + self.c} for v in (self.xp, self.xm))
        self.to_core = {'row': self.x * CORES + self.other}
        self.to_yp, self.to_ym = {'col': self.yp}, {'col': self.ym}
        self.to_lo = {'mpo': self.mpo + 1 - CORES * lax.rem(self.mpo, CORES)}
        self.to_hi = {'mpo': CHIPS - 1 - self.mpo}

    def turn(self, **steps):
        size = {'row': ROWS, 'col': CHIPS, 'mpo': CHIPS}
        return {a: lax.rem(getattr(self, a) + d, size[a]) for a, d in steps.items()}


def got(ref, send, recv, device):
    remote(ref, ref, send, recv, device).wait_recv()


class Ring:
    def __init__(self, me, at, first, send, recv):
        x, c, o = me.x, me.c, me.other
        whole = [(at(me.xm, c), me.to_core), (at(me.xp, c), me.to_core)]
        halves = [at(me.x2, c, h) for h in HALVES]
        self.moves = [(first, at(x, c), d) for d in (me.to_xp, me.to_xm, me.to_core)]
        self.moves += [(r, r, d) for r, d in (
            (at(me.xm, c, 0), me.to_xp), (at(me.xp, c, 1), me.to_xm), *whole, *((h, me.to_core) for h in halves))]
        self.lands = [at(me.xm, c), at(me.xp, c), at(x, o), *halves, at(me.xm, o), at(me.xp, o),
                      *(at(me.x2, o, h) for h in HALVES)]
        self.send, self.recv, self.device = send, recv, me.to_core

    def copy(self, k):
        return remote(*self.moves[k][:2], self.send.at[k], self.recv.at[k], self.moves[k][-1])

    def start(self, *ks):
        for k in ks:
            self.copy(k).start()

    def got(self, *ks):
        for k in ks:
            got(self.lands[k], self.send.at[k], self.recv.at[k], self.device)


(R_P, R_M, R_CORE, R_FWD_P, R_FWD_M, R_CORE_M, R_CORE_P, R_CORE_F0, R_CORE_F1) = range(9)


def setup_kernel(psi, left, right, w, hg, lg, rg, wg, st_psi, st_r, psi_s, psi_r, l1_s, l1_r, ly_s, ly_r, rz_s, rz_r,
                 rx_s, rx_r, rd_s, rd_r, w_s, w_r, loc):
    me = Around()
    row, col, mpo, c, o = me.row, me.col, me.mpo, me.c, me.other
    aw, bw, nb = psi.shape[0], psi.shape[-1], right.shape[-1]
    ah, bh, qa = aw // 2, bw // 2, aw // CHIPS
    half, zc, xc = nb // 2, nb // CHIPS, nb // (2 * ROWS)
    here = me.to_core
    plane = [(dr, dz) for dz in (2, 1, 3, 0) for dr in (4, 5, 2, 3, 6, 7, 1, 0)]

    bar = pltpu.get_barrier_semaphore()
    for dr, dz in plane[:-1]:
        signal(bar, me.turn(row=dr, mpo=dz))
    signal(bar, me.to_yp)
    signal(bar, me.to_ym)
    pl.semaphore_wait(bar, len(plane) + 1)

    for dr, dz in plane:
        to = me.turn(row=dr, mpo=dz)
        for l in HALVES:
            src = left.at[block(col * qa, qa), l, block(to['row'] * aw + hi_of(to['mpo']) * ah, ah)]
            dst = lg.at[mpo * 2 + l, row, col]
            if dr or dz:
                remote(src, dst, l1_s, l1_r, to).start()
            else:
                pltpu.make_async_copy(src, dst, l1_r).start()

    def r_rows(q, rl):
        return block((q * 2 + rl) * bh, bh)

    def r_src(z, rl, start, n):
        return right.at[block(lo_of(z) * bh, bh), rl, block(start, n)]

    def x_cols(x, core):
        return half + (x * CORES + core) * xc

    def r_part(g):
        return (x_cols(me.x, c), xc) if g == 0 else (c * zc, zc)

    def r_copies(g):
        for dz in FAR_FIRST:
            to = me.turn(mpo=dz)
            for rl in HALVES:
                sems = rz_s.at[dz - 1, rl, g], rz_r.at[dz - 1, rl, g]
                yield remote(r_src(to['mpo'], rl, *r_part(g)), rg.at[r_rows(CHIPS - dz, rl), block(*r_part(g))], *sems, to)

    def r_got(g):
        for dz in FAR_FIRST:
            for rl in HALVES:
                got(rg.at[r_rows(CHIPS - dz, rl), block(*r_part(g))], rz_s.at[dz - 1, rl, g], rz_r.at[dz - 1, rl, g], here)

    def w_copy(dz):
        return remote(w, wg.at[mpo], w_s.at[dz - 1], w_r.at[dz - 1], me.turn(mpo=dz))

    for copy in r_copies(0):
        copy.start()

    def psi_at(t):
        def at(x, core, h=None):
            start = (x * CORES + core) * aw
            return hg.at[t, block(start, aw) if h is None else block(start + h * ah, ah), :]
        return at

    def psi_src(t):
        return psi.at[:, t // 2, t % 2, block(me.lo * bh, bh)]

    slices = range(CHIPS)
    psi_rings = [Ring(me, psi_at(t), psi_src(t), psi_s.at[t], psi_r.at[t]) for t in slices]
    for ring in psi_rings:
        ring.start(R_P, R_M, R_CORE)
    for copy in r_copies(1):
        copy.start()
    for dz in OTHERS:
        w_copy(dz).start()

    own = [(w, wg.at[mpo], None)]
    own += [(psi_src(t), psi_at(t)(me.x, c), st_psi.at[t]) for t in slices]
    own += [(r_src(mpo, rl, 0, nb), rg.at[r_rows(0, rl), :], st_r.at[rl]) for rl in HALVES]
    for i, (src, dst, via) in enumerate(own):
        pltpu.make_async_copy(src, dst if via is None else via, loc.at[i]).start()
    for i, (src, dst, via) in enumerate(own):
        if via is not None:
            pltpu.make_async_copy(src, via, loc.at[i]).wait()
            pltpu.make_async_copy(via, dst, loc.at[i]).start()

    ls = range(2 * CHIPS)

    def l_at(y, h=None):
        return lg.at[0:len(ls) if h is None else CHIPS, :, y] if not h else lg.at[CHIPS:len(ls), :, y]

    ly_moves = [(l_at(col), me.to_yp), (l_at(col), me.to_ym), (l_at(me.ym, 0), me.to_yp), (l_at(me.yp, 1), me.to_ym)]
    ly = [remote(ref, ref, ly_s.at[k], ly_r.at[k], d) for k, (ref, d) in enumerate(ly_moves)]
    ly_lands = [l_at(me.ym), l_at(me.yp), l_at(me.y2, 0), l_at(me.y2, 1)]

    def ly_got(k):
        got(ly_lands[k], ly_s.at[k], ly_r.at[k], here)

    got(l_at(col), l1_s, l1_r, here)
    ly[0].start()
    ly[1].start()

    def rx_at(x, core, h=None):
        n = 6 * bh
        rows = pl.ds(2 * bh, n) if h is None else pl.ds(2 * bh + h * n // 2, n // 2)
        return rg.at[rows, block(x_cols(x, core), xc)]

    r_got(0)
    rx = Ring(me, rx_at, rx_at(me.x, c), rx_s, rx_r)
    rx.start(R_P, R_M, R_CORE)
    for ring in psi_rings:
        ring.got(R_P)
        ring.start(R_FWD_P, R_CORE_M)
        ring.got(R_M)
        ring.start(R_FWD_M, R_CORE_P)
    r_got(1)

    def rd_at(core):
        return rg.at[pl.ds(2 * bh, 6 * bh), block(core * zc, zc)]

    rd = remote(rd_at(c), rd_at(c), rd_s, rd_r, here)
    rd.start()
    rx.got(R_P)
    rx.start(R_FWD_P, R_CORE_M)
    rx.got(R_M)
    rx.start(R_FWD_M, R_CORE_P)
    for k in HALVES:
        ly_got(k)
        ly[2 + k].start()
    for ring in (*psi_rings, rx):
        ring.got(R_FWD_P)
        ring.start(R_CORE_F0)
        ring.got(R_FWD_M)
        ring.start(R_CORE_F1)
    for k in HALVES:
        ly_got(2 + k)

    for ring in (*psi_rings, rx):
        ring.got(R_CORE, R_CORE_M, R_CORE_P, R_CORE_F0, R_CORE_F1)
    got(rd_at(o), rd_s, rd_r, here)
    for dz in OTHERS:
        got(wg.at[lax.rem(mpo + CHIPS - dz, CHIPS)], w_s.at[dz - 1], w_r.at[dz - 1], here)
    for i, (src, dst, via) in enumerate(own):
        pltpu.make_async_copy(src if via is None else via, dst, loc.at[i]).wait()
    for ring in (*psi_rings, rx):
        for k in range(len(ring.moves)):
            ring.copy(k).wait_send()
    for copy in (*ly, *r_copies(0), *r_copies(1), *(w_copy(dz) for dz in OTHERS), rd):
        copy.wait_send()
    for ref in (lg.at[0:len(ls) - 1, :, 0], lg.at[0, 0:ROWS - 2, 0]):
        remote(ref, ref, l1_s, l1_r, here).wait_send()


def lanczos(hg, lt, rg, wg, out, ab, R, L, G, U, W3, T1, T2, TP, PY, RF, RN, RZ, V, AL, BE, BP, INV, ARS, AR1,
                 AR2, load, send, recv, ar1_s, ar1_r, ar2_s, ar2_r, credit, z_s, z_r, o_s):
    me = Around()
    row, col, mpo, x, c, hi, lo = me.row, me.col, me.mpo, me.x, me.c, me.hi, me.lo
    n_s, nb, bh = G.shape
    aw, bw = nb // ROWS, CORES * bh
    ah = aw // 2
    n_r, alt, o, last = 2 * CHIPS, 1 - hi, me.other, n_s - 1
    here, me2 = me.to_core, col * CHIPS + mpo
    slices, tile = range(n_s), AL.shape[0]
    others = [(dc, dz) for dc in range(CHIPS) for dz in range(CHIPS) if dc or dz]
    peers = [me.turn(row=d) for d in range(1, ROWS)] + [me.turn(col=dc, mpo=dz) for dc, dz in others]

    bar = pltpu.get_barrier_semaphore()
    for peer in peers:
        signal(bar, peer)

    def l_load(i, k):
        j = i % n_s
        return pltpu.make_async_copy(lt.at[pl.ds(i * ah, ah), k * bw:(k + 1) * bw], PY.at[j, k], load.at[j, k])

    n_k = range(nb // bw)
    for i in slices:
        for k in n_k:
            l_load(i, k).start()
    load_g, load_r = (pltpu.make_async_copy(src, dst, load.at[n_s, i]) for i, (src, dst) in enumerate(((hg, G), (rg, R))))
    load_g.start()
    load_r.start()

    U[...] = jnp.concatenate([wg[z][:, :U.shape[1] // CHIPS] for z in range(CHIPS)], axis=1)
    lane, sub = (lax.broadcasted_iota(jnp.int32, (tile, U.shape[1]), i) for i in (1, 0))
    diagonal = jnp.where(lax.rem(lane, tile) == sub, 1.0, 0.0)
    for t in slices:
        for r in range(0, n_r, 2):
            rows = [U[pl.ds(t * n_r + lax.rem(r + i + 2 * mpo, n_r), 1), :] * diagonal for i in HALVES]
            at = (t * n_r + r) * tile
            W3[at:at + 2 * tile] = jnp.concatenate(rows)
    for ref in (T2, TP, V, BP):
        ref[...] = jnp.zeros_like(ref)
    for i in range(n_r):
        for k in n_k:
            l_load(i, k).wait()
            L[i * ah:(i + 1) * ah, k * bw:(k + 1) * bw] = PY[i % n_s, k]
            if i < n_s:
                l_load(i + n_s, k).start()
    pl.semaphore_wait(bar, len(peers))
    load_g.wait()

    def rows_of(xx, cc, hh):
        return block((xx * CORES + cc) * aw + hh * ah, ah)

    own_rows = rows_of(x, c, hi)
    low, high = slice(0, bh), slice(bh, bw)

    def ends(k, t):
        def g_at(xx, cc, hh):
            return G.at[t, rows_of(xx, cc, hh), :]

        xp, xm, x2 = me.xp, me.xm, me.x2
        via = {
            HI: ((x, c, hi), (x, c, alt), me.to_hi),
            OWN_P: ((x, c, hi), (xm, c, hi), me.to_xp),
            OWN_M: ((x, c, hi), (xp, c, hi), me.to_xm),
            ALT_P: ((x, c, alt), (xm, c, alt), me.to_xp),
            ALT_M: ((x, c, alt), (xp, c, alt), me.to_xm),
            FWD_P: ((xm, c, hi), (x2, c, hi), me.to_xp),
            FWD_M: ((xp, c, alt), (x2, c, alt), me.to_xm),
        }
        for kind, xx, hh in ((OWN_D, x, hi), (ALT_D, x, alt), (DP_O, xp, hi), (DM_O, xm, hi), (DP_A, xp, alt),
                             (DM_A, xm, alt), (DF_O, x2, hi), (DF_A, x2, alt)):
            via[kind] = ((xx, c, hh), (xx, o, hh), me.to_core)
        if k in via:
            src, land, to = via[k]
            return g_at(*src), g_at(*src), g_at(*land), to
        far, plus, minus, own = (PY.at[t, i] for i in range(4))
        src, dst, to = {
            FAR_P: (far.at[:, low], RF.at[t, 0], me.to_yp),
            FAR_M: (far.at[:, high], RF.at[t, 1], me.to_ym),
            NEAR_P: (plus, RN.at[t, 0], me.to_yp),
            NEAR_M: (minus, RN.at[t, 1], me.to_ym),
            LO: (own.at[:, block((1 - lo) * bh, bh)], RZ.at[t], me.to_lo),
        }[k]
        return src, dst, dst, to

    def copy(k, t):
        src, dst, _, to = ends(k, t)
        return remote(src, dst, send.at[t, k], recv.at[t, k], to)

    def start(t, *kinds):
        for k in kinds:
            copy(k, t).start()

    def arrived(t, *kinds):
        for k in kinds:
            got(ends(k, t)[2], send.at[t, k], recv.at[t, k], here)

    def e1(t):
        start(t, FAR_P, FAR_M)

    def e2(t):
        arrived(t, FAR_P, FAR_M)
        PY[t, 1, :, low] += RF[t, 0]
        PY[t, 2, :, high] += RF[t, 1]
        start(t, NEAR_P, NEAR_M)

    def e3(t):
        arrived(t, NEAR_P, NEAR_M)
        PY[t, 3] += RN[t, 0] + RN[t, 1]
        start(t, LO)

    def e4(t):
        arrived(t, LO)
        G[t, own_rows, :] = PY[t, 3, :, block(lo * bh, bh)] + RZ[t]

    def g4(t):
        start(t, HI, OWN_P, OWN_M, OWN_D)

    def g5a(t):
        arrived(t, HI)
        start(t, ALT_P, ALT_M, ALT_D)

    def g5b(t):
        arrived(t, OWN_P)
        start(t, FWD_P, DM_O)
        arrived(t, OWN_M)
        start(t, DP_O)

    def g6a(t):
        arrived(t, ALT_M)
        start(t, FWD_M, DP_A)
        arrived(t, ALT_P)
        start(t, DM_A)

    def g6b(t):
        arrived(t, FWD_P)
        start(t, DF_O)

    def g7(t):
        arrived(t, FWD_M)
        start(t, DF_A)

    def ar_pair(k, stage):
        slots, s_sem, r_sem = ((AR1, ar1_s, ar1_r), (AR2, ar2_s, ar2_r))[stage]
        n = len(peers) - len(others) if stage == 0 else len(others)
        ref = slots.at[k, 0:n]
        return remote(ref, ref, s_sem.at[k], r_sem.at[k], here)

    def ar_send(k, stage, part):
        slots, s_sem, r_sem, mine = ((AR1, ar1_s, ar1_r, row), (AR2, ar2_s, ar2_r, me2))[stage]
        ARS[k, stage] = part
        slots[k, mine] = part
        first = len(peers) - len(others)
        for peer in (peers[first:] if stage else peers[:first]):
            remote(ARS.at[k, stage], slots.at[k, mine], s_sem.at[k], r_sem.at[k], peer).start()

    def ar_sum(k, stage):
        ar_pair(k, stage).wait_recv()
        slots = (AR1, AR2)[stage]
        return sum((slots[k, i] for i in range(1, slots.shape[1])), slots[k, 0])

    def ar_end(k):
        tot = jnp.sum(ar_sum(k, 1))
        for stage in HALVES:
            ar_pair(k, stage).wait_send()
        return tot

    def fold(v):
        v = jnp.sum(v.reshape(ah // tile, tile, bh), axis=0)
        n = ARS.shape[-1]
        return sum((v[:, i:i + n] for i in range(n, bh, n)), v[:, :n])

    def a1(j):
        p = lax.rem(j, 2)
        parts = [fold(V[p, t] * G[t, own_rows, :]) for t in slices]
        ar_send(0, 0, sum(parts[1:], parts[0]))

    def a2():
        ar_send(0, 1, ar_sum(0, 0))

    def a3(j):
        p = lax.rem(j, 2)
        AL[...] = jnp.full(AL.shape, ar_end(0), F32)
        al, bp, parts = AL[0:1, :], BP[0:1, :], []
        for t in slices:
            w = G[t, own_rows, :] - al * V[p, t] - bp * V[1 - p, t]
            V[1 - p, t] = w
            parts.append(fold(w * w))
        ar_send(1, 0, sum(parts[1:], parts[0]))

    def b2():
        ar_send(1, 1, ar_sum(1, 0))

    def b3(j):
        p = lax.rem(j, 2)
        BE[...] = jnp.sqrt(jnp.full(BE.shape, ar_end(1), F32))
        INV[...] = 1.0 / BE[...]
        for t in slices:
            V[1 - p, t] = V[1 - p, t] / BE[0:1, :]
        for i, ref in enumerate((AL, BE)):
            ab[i, j] = ref[:, :ab.shape[-1]]

    @pl.loop(0, STEPS)
    def _(j):
        later, more = j > 0, j < STEPS - 1

        def t1_tick(s, xx, first=False):
            ks = block(xx * CORES * aw, CORES * aw)
            n = n_r * ah // 2
            for m in HALVES:
                ms = slice(m * n, (m + 1) * n)
                d = dot_hi(L[ms, ks], G[s, ks, :])
                if first:
                    T1[s, ms] = d
                else:
                    T1[s, ms] += d

        @pl.loop(0, n_s)
        def _(s):
            @pl.when(later)
            def _():
                for t in (2, 3):
                    @pl.when(s == t - 2)
                    def _():
                        e3(t)

                arrived(s, OWN_D, ALT_D)

            @pl.when(s == last)
            def _():
                a3(j)

            t1_tick(s, x, True)

            @pl.when(later)
            def _():
                g6b(s)

                @pl.when(s < last)
                def _():
                    g5a(s + 1)

                arrived(s, DM_O, DM_A)

            @pl.when(s == 2)
            def _():
                a2()

            t1_tick(s, me.xm)

            @pl.when(later)
            def _():
                g7(s)

                @pl.when(s < last)
                def _():
                    g5b(s + 1)

                @pl.when(s < 2)
                def _():
                    e4(s + 2)
                    g4(s + 2)

                arrived(s, DP_O, DP_A)

            @pl.when(s == last)
            def _():
                b2()

            t1_tick(s, me.xp)

            @pl.when(later)
            def _():
                @pl.when(s < last)
                def _():
                    g6a(s + 1)

                arrived(s, DF_O, DF_A)

            @pl.when(s == 1)
            def _():
                a1(j)

            t1_tick(s, me.x2)

        @pl.when(later)
        def _():
            @pl.loop(0, n_s)
            def _(t):
                for k in range(N_COPY):
                    copy(k, t).wait_send()

        @pl.when(more)
        def _():
            for i, peer in enumerate((me.to_hi, me.to_xp, me.to_xm, me.to_core)):
                signal(credit.at[i], peer)

        b3(j)

        @pl.loop(0, ah // (4 * tile))
        def _(g):
            al, bp, inv = AL[...], BP[...], INV[...]
            for u in range(4):
                at_row = pl.multiple_of((g * 4 + u) * tile, tile)
                mixed = dot_hi(W3[...], jnp.concatenate(
                    [T1[s, pl.ds((2 * z + l) * ah + at_row, tile), :]
                     for z in range(CHIPS) for s in slices for l in HALVES]))
                for t in slices:
                    for r in range(n_r):
                        i = (t * n_r + r) * tile
                        at = (t, pl.ds(at_row, tile), slice(r * bh, (r + 1) * bh))
                        now = T2[at]
                        T2[at] = (mixed[i:i + tile] - al * now - bp * TP[at]) * inv
                        TP[at] = now

        BP[...] = BE[...]

        @pl.when(j == 0)
        def _():
            load_r.wait()

        def y_tick(t, which, yy):
            PY[t, which] = dot_hi(T2[t], R[:, block(yy * bw, bw)])

        def far(t):
            y_tick(t, 0, me.y2)
            e1(t)

        far(0)

        @pl.loop(0, n_s)
        def _(t):
            @pl.when(t < last)
            def _():
                far(t + 1)

            @pl.when(t == 2)
            def _():
                e4(0)

                @pl.when(more)
                def _():
                    for i in range(credit.shape[0]):
                        pl.semaphore_wait(credit.at[i], 1)
                    g4(0)

            @pl.when(jnp.logical_and(more, t == last))
            def _():
                g5a(0)

            y_tick(t, 1, me.yp)

            @pl.when(t == last)
            def _():
                e4(1)

                @pl.when(more)
                def _():
                    g5b(0)
                    g4(1)

            y_tick(t, 2, me.ym)
            e2(t)

            for i in HALVES:
                @pl.when(t == i + 1)
                def _():
                    e3(i)

            @pl.when(jnp.logical_and(more, t == last))
            def _():
                g6a(0)

            y_tick(t, 3, col)

    for t in (2, last):
        e3(t)
    for t in (2, last):
        e4(t)
    a1(STEPS)
    a2()
    a3(STEPS)
    b2()
    b3(STEPS)

    def out_at(z):
        return T1.at[:, block(lo_of(z) * aw + hi_of(z) * ah, ah), :]

    mine = out_at(mpo)
    T1[:, block(lo * aw + hi * ah, ah), :] = V[1 - STEPS % 2]

    def spread(dz):
        return remote(mine, mine, z_s.at[dz - 1], z_r.at[dz - 1], me.turn(mpo=dz))

    for dz in FAR_FIRST:
        spread(dz).start()
    for t in slices:
        for k in range(N_REDUCE):
            copy(k, t).wait_send()
    for dz in OTHERS:
        got(out_at(lax.rem(mpo + CHIPS - dz, CHIPS)), z_s.at[dz - 1], z_r.at[dz - 1], here)
    outs = [pltpu.make_async_copy(T1.at[t, h * aw:(h + 1) * aw, :], out.at[:, t // 2, t % 2, h * bh:(h + 1) * bh],
                                  o_s.at[t, h]) for t in slices for h in HALVES]
    for part in outs:
        part.start()
    for dz in OTHERS:
        spread(dz).wait_send()
    for part in outs:
        part.wait()


def solution(mesh):
    dma = pltpu.SemaphoreType.DMA
    anywhere, vmem = (pl.BlockSpec(memory_space=m) for m in (pl.ANY, pltpu.VMEM))

    def shape(*dims):
        return jax.ShapeDtypeStruct(dims, F32)

    def keep(*dims, dtype=F32):
        return pltpu.VMEM(dims, dtype)

    def local_fn(psi_blk, left_blk, right_blk, mpo_blk):
        aw, bw, nb = psi_blk.shape[0], psi_blk.shape[-1], right_blk.shape[-1]
        ah, bh, n_l, n_s = aw // 2, bw // 2, 2 * CHIPS, CHIPS
        tile, lanes = 8, min(128, bh)
        w = mpo_blk.reshape(2, n_l, n_s, n_s).transpose(3, 1, 2, 0).reshape(n_s * n_l, n_l)
        w = jnp.pad(jnp.repeat(w, tile, axis=1), ((0, 0), (0, n_l * tile)))
        two, nine, far = dma((2,)), dma((9,)), dma((3,))
        hg, lg, rg, wg = pl.pallas_call(
            setup_kernel,
            out_shape=(shape(n_s, nb, bh), shape(n_l, ROWS, CHIPS, aw // CHIPS, ah), shape(n_l * bh, nb),
                       shape(CHIPS, *w.shape)),
            in_specs=[anywhere] * 4,
            out_specs=[anywhere] * 4,
            scratch_shapes=[
                keep(n_s, aw, bh), keep(2, bh, nb), dma((n_s, 9)), dma((n_s, 9)), dma, dma, dma((4,)), dma((4,)),
                dma((3, 2, 2)), dma((3, 2, 2)), nine, nine, dma, dma, far, far, dma((7,)),
            ],
            compiler_params=pltpu.CompilerParams(collective_id=0, has_side_effects=True),
            name='setup',
        )(psi_blk, left_blk, right_blk, w)

        lt = lg.reshape(n_l, nb, ah).transpose(0, 2, 1).reshape(n_l * ah, nb)
        v_next, ab = pl.pallas_call(
            lanczos,
            out_shape=(shape(*psi_blk.shape), shape(2, STEPS + 1, tile, lanes)),
            in_specs=[anywhere, anywhere, anywhere, vmem],
            out_specs=[anywhere, vmem],
            scratch_shapes=[
                keep(n_l * bh, nb), keep(n_l * ah, nb), keep(n_s, nb, bh), keep(n_s * n_l, 256),
                keep(256, 256), keep(n_s, n_l * ah, bh), keep(n_s, ah, n_l * bh),
                keep(n_s, ah, n_l * bh), keep(n_s, 4, ah, bw), keep(n_s, 2, ah, bh), keep(n_s, 2, ah, bw),
                keep(n_s, ah, bh), keep(2, n_s, ah, bh), *[keep(tile, bh)] * 4,
                keep(2, 2, tile, lanes), keep(2, ROWS, tile, lanes), keep(2, CHIPS * CHIPS, tile, lanes),
                dma((n_s + 1, 4)), dma((n_s, N_COPY)), dma((n_s, N_COPY)), two, two, two, two,
                pltpu.SemaphoreType.REGULAR((4,)), far, far, dma((n_s, 2)),
            ],
            compiler_params=pltpu.CompilerParams(collective_id=1, has_side_effects=True, vmem_limit_bytes=62 * MIB),
            name='lanczos',
        )(hg, lt, rg, wg)
        return ab[0, 1:, 0, 0], ab[1, 1:, 0, 0], v_next

    return jax.shard_map(
        local_fn,
        mesh=mesh,
        in_specs=(P('row', None, None, 'col'), P('row', 'mpo', None), P('col', 'mpo', None),
                  P('mpo', None, None, None, None, None)),
        out_specs=(P(), P(), P('row', None, None, 'col')),
        check_vma=False,
    )
```

```python
import jax
import jax.numpy as jnp
from jax import lax
from jax.experimental import pallas as pl
from jax.experimental.pallas import tpu as pltpu
from jax.sharding import PartitionSpec as P

STEPS = 4
F32 = jnp.float32
MIB = 2**20


(FAR_P, FAR_M, NEAR_P, NEAR_M, LO, HI, OWN_P, OWN_M, OWN_D, ALT_P, ALT_M, ALT_D, FWD_P, DP_O, DM_O, DP_A, DM_A,
 FWD_M, DF_O, DF_A) = range(20)
N_COPY, N_REDUCE = 20, 5


HALVES = (0, 1)
OTHERS = (1, 2, 3)
FAR_FIRST = (2, 1, 3)
CHIPS, CORES, ROWS = 4, 2, 8


def dot_hi(a, b):
    return lax.dot_general(a, b, (((1,), (0,)), ((), ())), precision=lax.Precision.HIGHEST, preferred_element_type=F32)


def hi_of(z):
    return lax.div(z, 2)


def lo_of(z):
    return lax.rem(lax.div(z + 1, 2), 2)


def remote(src, dst, send, recv, device):
    return pltpu.make_async_remote_copy(src_ref=src, dst_ref=dst, send_sem=send, recv_sem=recv, device_id=device,
                                        device_id_type=pl.DeviceIdType.MESH)


def signal(sem, device):
    pl.semaphore_signal(sem, inc=1, device_id=device, device_id_type=pl.DeviceIdType.MESH)


def block(start, n):
    return pl.ds(pl.multiple_of(start, n), n)


class Around:
    def __init__(self):
        self.row, self.col, self.mpo = (lax.axis_index(a) for a in ('row', 'col', 'mpo'))
        self.x, self.c = lax.div(self.row, CORES), lax.rem(self.row, CORES)
        self.hi, self.lo = hi_of(self.mpo), lo_of(self.mpo)
        (self.xp, self.x2, self.xm), (self.yp, self.y2, self.ym) = (
            [lax.rem(v + d, CHIPS) for d in OTHERS] for v in (self.x, self.col))
        self.other = 1 - self.c
        self.to_xp, self.to_xm = ({'row': v * CORES + self.c} for v in (self.xp, self.xm))
        self.to_core = {'row': self.x * CORES + self.other}
        self.to_yp, self.to_ym = {'col': self.yp}, {'col': self.ym}
        self.to_lo = {'mpo': self.mpo + 1 - CORES * lax.rem(self.mpo, CORES)}
        self.to_hi = {'mpo': CHIPS - 1 - self.mpo}

    def turn(self, **steps):
        size = {'row': ROWS, 'col': CHIPS, 'mpo': CHIPS}
        return {a: lax.rem(getattr(self, a) + d, size[a]) for a, d in steps.items()}


def got(ref, send, recv, device):
    remote(ref, ref, send, recv, device).wait_recv()


class Ring:
    def __init__(self, me, at, first, send, recv):
        x, c, o = me.x, me.c, me.other
        whole = [(at(me.xm, c), me.to_core), (at(me.xp, c), me.to_core)]
        halves = [at(me.x2, c, h) for h in HALVES]
        self.moves = [(first, at(x, c), d) for d in (me.to_xp, me.to_xm, me.to_core)]
        self.moves += [(r, r, d) for r, d in (
            (at(me.xm, c, 0), me.to_xp), (at(me.xp, c, 1), me.to_xm), *whole, *((h, me.to_core) for h in halves))]
        self.lands = [at(me.xm, c), at(me.xp, c), at(x, o), *halves, at(me.xm, o), at(me.xp, o),
                      *(at(me.x2, o, h) for h in HALVES)]
        self.send, self.recv, self.device = send, recv, me.to_core

    def copy(self, k):
        return remote(*self.moves[k][:2], self.send.at[k], self.recv.at[k], self.moves[k][-1])

    def start(self, *ks):
        for k in ks:
            self.copy(k).start()

    def sent(self):
        for k in range(len(self.moves)):
            self.copy(k).wait_send()

    def got(self, *ks):
        for k in ks:
            got(self.lands[k], self.send.at[k], self.recv.at[k], self.device)


(R_P, R_M, R_CORE, R_FWD_P, R_FWD_M, R_CORE_M, R_CORE_P, R_CORE_F0, R_CORE_F1) = range(9)


def lanczos(psi, left, right, w, out, ab, R, L, G, WG, U, W3, T1, T2, TP, PY, RF, RN, RZ, V, AL, BE, BP, INV, ARS, AR1,
            AR2, l_s, l_r, ly_s, ly_r, psi_s, psi_r, rz_s, rz_r, rx_s, rx_r, rd_s, rd_r, w_s, w_r, local, send, recv,
            ar1_s, ar1_r, ar2_s, ar2_r, credit, z_free, z_s, z_r, o_s):
    me = Around()
    row, col, mpo, x, c, hi, lo = me.row, me.col, me.mpo, me.x, me.c, me.hi, me.lo
    n_s, nb, bh = G.shape
    aw, bw = nb // ROWS, CORES * bh
    ah = aw // 2
    n_r, alt, o, last = 2 * CHIPS, 1 - hi, me.other, n_s - 1
    here, me2 = me.to_core, col * CHIPS + mpo
    slices, tile = range(n_s), AL.shape[0]
    others = [(dc, dz) for dc in range(CHIPS) for dz in range(CHIPS) if dc or dz]
    peers = [me.turn(row=d) for d in range(1, ROWS)] + [me.turn(col=dc, mpo=dz) for dc, dz in others]
    plane = [(dr, dz) for dz in (*FAR_FIRST, 0) for dr in (4, 5, 2, 3, 6, 7, 1, 0)]

    bar = pltpu.get_barrier_semaphore()
    greeted = [me.turn(row=dr, mpo=dz) for dr, dz in plane[:-1]] + [me.turn(col=dc, mpo=dz) for dc, dz in others if dc]
    for peer in greeted:
        signal(bar, peer)
    pl.semaphore_wait(bar, len(greeted))

    wide = ROWS * ah
    q_even, q_odd = aw // CHIPS, ah // CHIPS

    def l_parts(z, y, first, n):
        def lanes(h):
            return pl.ds(pl.multiple_of(h * wide + first, ah), n)

        return (T2.at[z, block(lax.rem(y, 2) * q_even, q_even), lanes(lax.div(y, 2))],
                TP.at[z, block(y * q_odd, q_odd), lanes(0)], TP.at[z, :, lanes(1)])

    n_kinds = range(3)
    for kind in n_kinds:
        for dr, dz in plane:
            to = me.turn(row=dr, mpo=dz)
            cols = block(to['row'] * aw + hi_of(to['mpo']) * ah, ah)
            rows = (block(col * q_even, q_even), block(col * q_odd, q_odd), pl.ds(ah, ah))[kind]
            src = left.at[rows, min(kind, 1), cols]
            dst = l_parts(mpo, col, row * ah, ah)[kind]
            if dr or dz:
                remote(src, dst, l_s.at[kind], l_r.at[kind], to).start()
            else:
                pltpu.make_async_copy(src, dst, l_r.at[kind]).start()
        if kind == 1:
            def psi_at(t):
                def at(xx, core, h=None):
                    first = (xx * CORES + core) * aw
                    return G.at[t, block(first, aw) if h is None else block(first + h * ah, ah), :]
                return at

            def psi_src(t):
                return psi.at[:, t // 2, t % 2, block(lo * bh, bh)]

            psi_rings = [Ring(me, psi_at(t), psi_src(t), psi_s.at[t], psi_r.at[t]) for t in slices]
            for ring in psi_rings:
                ring.start(R_P, R_M, R_CORE)

    half, zc, xc = nb // 2, nb // CHIPS, nb // (2 * ROWS)

    def r_rows(q, rl):
        return block((q * 2 + rl) * bh, bh)

    def r_src(z, rl, first, n):
        return right.at[block(lo_of(z) * bh, bh), rl, block(first, n)]

    def x_cols(xx, core):
        return half + (xx * CORES + core) * xc

    def r_part(g):
        return (x_cols(x, c), xc) if g == 0 else (c * zc, zc)

    def r_copies(g):
        for dz in FAR_FIRST:
            to = me.turn(mpo=dz)
            for rl in HALVES:
                sems = rz_s.at[dz - 1, rl, g], rz_r.at[dz - 1, rl, g]
                yield remote(r_src(to['mpo'], rl, *r_part(g)), R.at[r_rows(CHIPS - dz, rl), block(*r_part(g))], *sems, to)

    def r_got(g):
        for dz in FAR_FIRST:
            for rl in HALVES:
                got(R.at[r_rows(CHIPS - dz, rl), block(*r_part(g))], rz_s.at[dz - 1, rl, g], rz_r.at[dz - 1, rl, g], here)

    def rx_at(xx, core, h=None):
        n = (n_r - 2) * bh
        rows = pl.ds(2 * bh, n) if h is None else pl.ds(2 * bh + h * n // 2, n // 2)
        return R.at[rows, block(x_cols(xx, core), xc)]

    rx = Ring(me, rx_at, rx_at(x, c), rx_s, rx_r)

    def rd_at(core):
        return R.at[pl.ds(2 * bh, (n_r - 2) * bh), block(core * zc, zc)]

    rd = remote(rd_at(c), rd_at(c), rd_s, rd_r, here)

    def w_copy(dz):
        return remote(w, WG.at[mpo], w_s.at[dz - 1], w_r.at[dz - 1], me.turn(mpo=dz))

    for dz in OTHERS:
        w_copy(dz).start()
    for g in HALVES:
        for part in r_copies(g):
            part.start()

    own = [(w, WG.at[mpo])] + [(psi_src(t), psi_at(t)(x, c)) for t in slices]
    own += [(r_src(mpo, rl, 0, nb), R.at[r_rows(0, rl), :]) for rl in HALVES]
    own = [pltpu.make_async_copy(src, dst, local.at[i]) for i, (src, dst) in enumerate(own)]
    for part in own:
        part.start()

    for ref in (V, BP):
        ref[...] = jnp.zeros_like(ref)

    def quarter(y, h=None):
        zs = slice(0, CHIPS) if h is None else slice(2 * h, 2 * h + 2)
        return [ref.at[zs] for ref in (T2.at[:, block(lax.rem(y, 2) * q_even, q_even), block(lax.div(y, 2) * wide, wide)],
                                       TP.at[:, block(y * q_odd, q_odd), pl.ds(0, wide)])]

    def ly(k):
        refs, to = ((quarter(col), me.to_yp), (quarter(col), me.to_ym), (quarter(me.ym, 0), me.to_yp),
                    (quarter(me.yp, 1), me.to_ym))[k]
        return [remote(ref, ref, ly_s.at[k, i], ly_r.at[k, i], to) for i, ref in enumerate(refs)]

    def ly_start(*ks):
        for k in ks:
            for part in ly(k):
                part.start()

    def ly_got(k):
        refs = (quarter(me.ym), quarter(me.yp), quarter(me.y2, 0), quarter(me.y2, 1))[k]
        for i, ref in enumerate(refs):
            got(ref, ly_s.at[k, i], ly_r.at[k, i], here)

    for kind, ref in enumerate(quarter(col)):
        got(ref, l_s.at[kind], l_r.at[kind], here)
    ly_start(0, 1)
    for k in HALVES:
        ly_got(k)
        ly_start(k + 2)
    for ring in psi_rings:
        ring.got(R_P)
        ring.start(R_FWD_P, R_CORE_M)
        ring.got(R_M)
        ring.start(R_FWD_M, R_CORE_P)
    r_got(0)
    rx.start(R_P, R_M, R_CORE)

    for dz in OTHERS:
        got(WG.at[lax.rem(mpo + CHIPS - dz, CHIPS)], w_s.at[dz - 1], w_r.at[dz - 1], here)
    own[0].wait()
    U[...] = jnp.concatenate([WG[z][:, :U.shape[1] // CHIPS] for z in range(CHIPS)], axis=1)
    lane, sub = (lax.broadcasted_iota(jnp.int32, (tile, U.shape[1]), i) for i in (1, 0))
    diagonal = jnp.where(lax.rem(lane, tile) == sub, 1.0, 0.0)
    for t in slices:
        for r in range(n_r):
            at = (t * n_r + r) * tile
            W3[at:at + tile] = U[pl.ds(t * n_r + lax.rem(r + 2 * mpo, n_r), 1), :] * diagonal

    for ring in psi_rings:
        ring.got(R_FWD_P)
        ring.start(R_CORE_F0)
        ring.got(R_FWD_M)
        ring.start(R_CORE_F1)
    got(TP.at[:, :, pl.ds(wide, wide)], l_s.at[2], l_r.at[2], here)
    for k in HALVES:
        ly_got(k + 2)
    for k in range(CHIPS):
        for part in ly(k):
            part.wait_send()

    @pl.loop(0, CHIPS)
    def _(z):
        for l, ref in enumerate((T2, TP)):
            for h in HALVES:
                for rr in range(ROWS):
                    first = h * wide + rr * ah
                    L[block((2 * z + l) * ah, ah), rr * aw + h * ah:rr * aw + (h + 1) * ah] = ref[z, :, first:first + ah].T

    for ref in (T2, TP):
        ref[...] = jnp.zeros_like(ref)
    for ring in psi_rings:
        ring.got(R_CORE, R_CORE_M, R_CORE_P, R_CORE_F0, R_CORE_F1)
    for part in own[1:1 + n_s]:
        part.wait()
    for ring in psi_rings:
        ring.sent()

    def r_round():
        rx.got(R_P)
        rx.start(R_FWD_P, R_CORE_M)
        rx.got(R_M)
        rx.start(R_FWD_M, R_CORE_P)

    def r_cores():
        r_got(1)
        rd.start()

    def r_far():
        rx.got(R_FWD_P)
        rx.start(R_CORE_F0)
        rx.got(R_FWD_M)
        rx.start(R_CORE_F1)

    def r_end():
        rx.got(R_CORE, R_CORE_M, R_CORE_P, R_CORE_F0, R_CORE_F1)
        got(rd_at(o), rd_s, rd_r, here)
        for part in own[1 + n_s:]:
            part.wait()
        rx.sent()
        for part in (*r_copies(0), *r_copies(1), *(w_copy(dz) for dz in OTHERS), rd):
            part.wait_send()
        for kind in n_kinds:
            for z, n in ((slice(0, CHIPS - 1), wide), (0, wide - ah)):
                ref = l_parts(z, col, 0, n)[kind]
                remote(ref, ref, l_s.at[kind], l_r.at[kind], here).wait_send()

    def rows_of(xx, cc, hh):
        return block((xx * CORES + cc) * aw + hh * ah, ah)

    own_rows = rows_of(x, c, hi)
    low, high = slice(0, bh), slice(bh, bw)

    def ends(k, t):
        def g_at(xx, cc, hh):
            return G.at[t, rows_of(xx, cc, hh), :]

        xp, xm, x2 = me.xp, me.xm, me.x2
        via = {
            HI: ((x, c, hi), (x, c, alt), me.to_hi),
            OWN_P: ((x, c, hi), (xm, c, hi), me.to_xp),
            OWN_M: ((x, c, hi), (xp, c, hi), me.to_xm),
            ALT_P: ((x, c, alt), (xm, c, alt), me.to_xp),
            ALT_M: ((x, c, alt), (xp, c, alt), me.to_xm),
            FWD_P: ((xm, c, hi), (x2, c, hi), me.to_xp),
            FWD_M: ((xp, c, alt), (x2, c, alt), me.to_xm),
        }
        for kind, xx, hh in ((OWN_D, x, hi), (ALT_D, x, alt), (DP_O, xp, hi), (DM_O, xm, hi), (DP_A, xp, alt),
                             (DM_A, xm, alt), (DF_O, x2, hi), (DF_A, x2, alt)):
            via[kind] = ((xx, c, hh), (xx, o, hh), me.to_core)
        if k in via:
            src, land, to = via[k]
            return g_at(*src), g_at(*src), g_at(*land), to
        far, plus, minus, own = (PY.at[t, i] for i in range(4))
        src, dst, to = {
            FAR_P: (far.at[:, low], RF.at[t, 0], me.to_yp),
            FAR_M: (far.at[:, high], RF.at[t, 1], me.to_ym),
            NEAR_P: (plus, RN.at[t, 0], me.to_yp),
            NEAR_M: (minus, RN.at[t, 1], me.to_ym),
            LO: (own.at[:, block((1 - lo) * bh, bh)], RZ.at[t], me.to_lo),
        }[k]
        return src, dst, dst, to

    def copy(k, t):
        src, dst, _, to = ends(k, t)
        return remote(src, dst, send.at[t, k], recv.at[t, k], to)

    def start(t, *kinds):
        for k in kinds:
            copy(k, t).start()

    def arrived(t, *kinds):
        for k in kinds:
            got(ends(k, t)[2], send.at[t, k], recv.at[t, k], here)

    def e1(t):
        start(t, FAR_P, FAR_M)

    def e2(t):
        arrived(t, FAR_P, FAR_M)
        PY[t, 1, :, low] += RF[t, 0]
        PY[t, 2, :, high] += RF[t, 1]
        start(t, NEAR_P, NEAR_M)

    def e3(t):
        arrived(t, NEAR_P, NEAR_M)
        PY[t, 3] += RN[t, 0] + RN[t, 1]
        start(t, LO)

    def e4(t):
        arrived(t, LO)
        G[t, own_rows, :] = PY[t, 3, :, block(lo * bh, bh)] + RZ[t]

    def g4(t):
        start(t, HI, OWN_P, OWN_M, OWN_D)

    def g5a(t):
        arrived(t, HI)
        start(t, ALT_P, ALT_M, ALT_D)

    def g5b(t):
        arrived(t, OWN_P)
        start(t, FWD_P, DM_O)
        arrived(t, OWN_M)
        start(t, DP_O)

    def g6a(t):
        arrived(t, ALT_M)
        start(t, FWD_M, DP_A)
        arrived(t, ALT_P)
        start(t, DM_A)

    def g6b(t):
        arrived(t, FWD_P)
        start(t, DF_O)

    def g7(t):
        arrived(t, FWD_M)
        start(t, DF_A)

    newest, oldest = STEPS % 2, 1 - STEPS % 2

    def z_copy(i, t, dz):
        src = (RZ.at[t], V.at[newest, t])[i]
        dst = TP.at[t, :, block((i * len(OTHERS) + dz - 1) * bh, bh)]
        return remote(src, dst, z_s.at[i, t, dz - 1], z_r.at[i, t, dz - 1], me.turn(mpo=dz))

    def z_start(i, t):
        for dz in FAR_FIRST:
            z_copy(i, t, dz).start()

    def share(t):
        RZ[t] = G[t, own_rows, :] - BP[0:1, :] * V[oldest, t]
        z_start(0, t)

    def ar_pair(k, stage):
        slots, s_sem, r_sem = ((AR1, ar1_s, ar1_r), (AR2, ar2_s, ar2_r))[stage]
        n = len(peers) - len(others) if stage == 0 else len(others)
        ref = slots.at[k, 0:n]
        return remote(ref, ref, s_sem.at[k], r_sem.at[k], here)

    def ar_send(k, stage, part):
        slots, s_sem, r_sem, mine = ((AR1, ar1_s, ar1_r, row), (AR2, ar2_s, ar2_r, me2))[stage]
        ARS[k, stage] = part
        slots[k, mine] = part
        first = len(peers) - len(others)
        for peer in (peers[first:] if stage else peers[:first]):
            remote(ARS.at[k, stage], slots.at[k, mine], s_sem.at[k], r_sem.at[k], peer).start()

    def ar_sum(k, stage):
        ar_pair(k, stage).wait_recv()
        slots = (AR1, AR2)[stage]
        return sum((slots[k, i] for i in range(1, slots.shape[1])), slots[k, 0])

    def ar_end(k):
        tot = jnp.sum(ar_sum(k, 1))
        for stage in HALVES:
            ar_pair(k, stage).wait_send()
        return tot

    def fold(v):
        v = jnp.sum(v.reshape(ah // tile, tile, bh), axis=0)
        n = ARS.shape[-1]
        return sum((v[:, i:i + n] for i in range(n, bh, n)), v[:, :n])

    def a1(j):
        p = lax.rem(j, 2)
        parts = [fold(V[p, t] * G[t, own_rows, :]) for t in slices]
        ar_send(0, 0, sum(parts[1:], parts[0]))

    def a2():
        ar_send(0, 1, ar_sum(0, 0))

    def a3(j):
        p = lax.rem(j, 2)
        AL[...] = jnp.full(AL.shape, ar_end(0), F32)
        al, bp, parts = AL[0:1, :], BP[0:1, :], []
        for t in slices:
            w = (G[t, own_rows, :] - bp * V[1 - p, t]) - al * V[p, t]
            V[1 - p, t] = w
            parts.append(fold(w * w))
        ar_send(1, 0, sum(parts[1:], parts[0]))

    def b2():
        ar_send(1, 1, ar_sum(1, 0))

    def b3(j):
        p = lax.rem(j, 2)
        BE[...] = jnp.sqrt(jnp.full(BE.shape, ar_end(1), F32))
        INV[...] = 1.0 / BE[...]
        for t in slices:
            V[1 - p, t] = V[1 - p, t] / BE[0:1, :]
        for i, ref in enumerate((AL, BE)):
            ab[i, j] = ref[:, :ab.shape[-1]]

    @pl.loop(0, STEPS)
    def _(j):
        first, later, more = j == 0, j > 0, j < STEPS - 1

        def t1_tick(s, xx, new=False):
            ks = block(xx * CORES * aw, CORES * aw)
            n = n_r * ah // 2
            for m in HALVES:
                ms = slice(m * n, (m + 1) * n)
                d = dot_hi(L[ms, ks], G[s, ks, :])
                if new:
                    T1[s, ms] = d
                else:
                    T1[s, ms] += d

        @pl.loop(0, n_s)
        def _(s):
            @pl.when(later)
            def _():
                for t in (2, 3):
                    @pl.when(s == t - 2)
                    def _():
                        e3(t)

                arrived(s, OWN_D, ALT_D)

            @pl.when(s == last)
            def _():
                a3(j)

            t1_tick(s, x, True)

            @pl.when(later)
            def _():
                g6b(s)

                @pl.when(s < last)
                def _():
                    g5a(s + 1)

                arrived(s, DM_O, DM_A)

            @pl.when(s == 2)
            def _():
                a2()

            for i, event in enumerate((r_cores, r_round, r_far)):
                @pl.when(jnp.logical_and(first, s == i + 1))
                def _():
                    event()

            t1_tick(s, me.xm)

            @pl.when(later)
            def _():
                g7(s)

                @pl.when(s < last)
                def _():
                    g5b(s + 1)

                @pl.when(s < 2)
                def _():
                    e4(s + 2)
                    g4(s + 2)

                arrived(s, DP_O, DP_A)

            @pl.when(s == last)
            def _():
                b2()

            t1_tick(s, me.xp)

            @pl.when(later)
            def _():
                @pl.when(s < last)
                def _():
                    g6a(s + 1)

                arrived(s, DF_O, DF_A)

            @pl.when(s == 1)
            def _():
                a1(j)

            t1_tick(s, me.x2)

        @pl.when(later)
        def _():
            @pl.loop(0, n_s)
            def _(t):
                for k in range(N_COPY):
                    copy(k, t).wait_send()

        @pl.when(more)
        def _():
            for i, peer in enumerate((me.to_hi, me.to_xp, me.to_xm, me.to_core)):
                signal(credit.at[i], peer)

        b3(j)

        @pl.loop(0, ah // (4 * tile))
        def _(g):
            al, bp, inv = AL[...], BP[...], INV[...]
            for u in range(4):
                at_row = pl.multiple_of((g * 4 + u) * tile, tile)
                mixed = dot_hi(W3[...], jnp.concatenate(
                    [T1[s, pl.ds((2 * z + l) * ah + at_row, tile), :]
                     for z in range(CHIPS) for s in slices for l in HALVES]))
                for t in slices:
                    for r in range(n_r):
                        i = (t * n_r + r) * tile
                        at = (t, pl.ds(at_row, tile), slice(r * bh, (r + 1) * bh))
                        now = T2[at]
                        T2[at] = (mixed[i:i + tile] - al * now - bp * TP[at]) * inv
                        TP[at] = now

        BP[...] = BE[...]

        @pl.when(jnp.logical_not(more))
        def _():
            for dz in OTHERS:
                signal(z_free.at[dz - 1], me.turn(mpo=dz))

        @pl.when(first)
        def _():
            r_end()

        def y_tick(t, which, yy):
            PY[t, which] = dot_hi(T2[t], R[:, block(yy * bw, bw)])

        def far(t):
            y_tick(t, 0, me.y2)
            e1(t)

        far(0)

        @pl.loop(0, n_s)
        def _(t):
            @pl.when(jnp.logical_and(jnp.logical_not(more), t == 0))
            def _():
                for dz in OTHERS:
                    pl.semaphore_wait(z_free.at[dz - 1], 1)

            @pl.when(jnp.logical_not(more))
            def _():
                z_start(1, t)

            @pl.when(t < last)
            def _():
                far(t + 1)

            @pl.when(t == 2)
            def _():
                e4(0)

                @pl.when(more)
                def _():
                    for i in range(credit.shape[0]):
                        pl.semaphore_wait(credit.at[i], 1)
                    g4(0)

                @pl.when(jnp.logical_not(more))
                def _():
                    share(0)

            @pl.when(jnp.logical_and(more, t == last))
            def _():
                g5a(0)

            y_tick(t, 1, me.yp)

            @pl.when(t == last)
            def _():
                e4(1)

                @pl.when(more)
                def _():
                    g5b(0)
                    g4(1)

                @pl.when(jnp.logical_not(more))
                def _():
                    share(1)

            y_tick(t, 2, me.ym)
            e2(t)

            for i in HALVES:
                @pl.when(t == i + 1)
                def _():
                    e3(i)

            @pl.when(jnp.logical_and(more, t == last))
            def _():
                g6a(0)

            y_tick(t, 3, col)

    for t in (2, last):
        e3(t)
    for t in (2, last):
        e4(t)
        share(t)
    a1(STEPS)
    a2()
    a3(STEPS)
    b2()
    for t in slices:
        for i in HALVES:
            for dz in OTHERS:
                got(TP.at[t, :, block((i * len(OTHERS) + dz - 1) * bh, bh)], z_s.at[i, t, dz - 1], z_r.at[i, t, dz - 1], here)
    b3(STEPS)

    def out_at(z):
        return block(lo_of(z) * aw + hi_of(z) * ah, ah)

    al, be = AL[0:1, :], BE[0:1, :]
    for t in slices:
        T1[t, out_at(mpo), :] = V[oldest, t]
        for dz in OTHERS:
            g, v = (TP[t, :, block((i * len(OTHERS) + dz - 1) * bh, bh)] for i in HALVES)
            T1[t, out_at(lax.rem(mpo + CHIPS - dz, CHIPS)), :] = (g - al * v) / be
        for h in HALVES:
            pltpu.make_async_copy(T1.at[t, h * aw:(h + 1) * aw, :], out.at[:, t // 2, t % 2, h * bh:(h + 1) * bh],
                                  o_s.at[t, h]).start()
    for t in slices:
        for k in range(N_REDUCE):
            copy(k, t).wait_send()
        for i in HALVES:
            for dz in OTHERS:
                z_copy(i, t, dz).wait_send()
        for h in HALVES:
            pltpu.make_async_copy(T1.at[t, h * aw:(h + 1) * aw, :], out.at[:, t // 2, t % 2, h * bh:(h + 1) * bh],
                                  o_s.at[t, h]).wait()


def solution(mesh):
    dma = pltpu.SemaphoreType.DMA
    anywhere, vmem = (pl.BlockSpec(memory_space=m) for m in (pl.ANY, pltpu.VMEM))

    def shape(*dims):
        return jax.ShapeDtypeStruct(dims, F32)

    def keep(*dims, dtype=F32):
        return pltpu.VMEM(dims, dtype)

    def local_fn(psi_blk, left_blk, right_blk, mpo_blk):
        aw, bw, nb = psi_blk.shape[0], psi_blk.shape[-1], right_blk.shape[-1]
        ah, bh, n_l, n_s = aw // 2, bw // 2, 2 * CHIPS, CHIPS
        tile, lanes = 8, min(128, bh)
        w = mpo_blk.reshape(2, n_l, n_s, n_s).transpose(3, 1, 2, 0).reshape(n_s * n_l, n_l)
        w = jnp.pad(jnp.repeat(w, tile, axis=1), ((0, 0), (0, n_l * tile)))
        two, nine, far = dma((2,)), dma((9,)), dma((3,))
        v_next, ab = pl.pallas_call(
            lanczos,
            out_shape=(shape(*psi_blk.shape), shape(2, STEPS + 1, tile, lanes)),
            in_specs=[anywhere] * 4,
            out_specs=[anywhere, vmem],
            scratch_shapes=[
                keep(n_l * bh, nb), keep(n_l * ah, nb), keep(n_s, nb, bh), keep(CHIPS, *w.shape), keep(n_s * n_l, 256),
                keep(256, 256), keep(n_s, n_l * ah, bh), keep(n_s, ah, n_l * bh), keep(n_s, ah, n_l * bh),
                keep(n_s, 4, ah, bw), keep(n_s, 2, ah, bh), keep(n_s, 2, ah, bw), keep(n_s, ah, bh),
                keep(2, n_s, ah, bh), *[keep(tile, bh)] * 4,
                keep(2, 2, tile, lanes), keep(2, ROWS, tile, lanes), keep(2, CHIPS * CHIPS, tile, lanes),
                far, far, dma((4, 2)), dma((4, 2)), dma((n_s, 9)), dma((n_s, 9)), dma((3, 2, 2)), dma((3, 2, 2)),
                nine, nine, dma, dma, far, far, dma((7,)),
                dma((n_s, N_COPY)), dma((n_s, N_COPY)), two, two, two, two,
                pltpu.SemaphoreType.REGULAR((4,)), pltpu.SemaphoreType.REGULAR((3,)), dma((2, n_s, 3)), dma((2, n_s, 3)),
                dma((n_s, 2)),
            ],
            compiler_params=pltpu.CompilerParams(collective_id=0, has_side_effects=True, vmem_limit_bytes=62 * MIB),
            name='lanczos',
        )(psi_blk, left_blk, right_blk, w)
        return ab[0, 1:, 0, 0], ab[1, 1:, 0, 0], v_next

    return jax.shard_map(
        local_fn,
        mesh=mesh,
        in_specs=(P('row', None, None, 'col'), P('row', 'mpo', None), P('col', 'mpo', None),
                  P('mpo', None, None, None, None, None)),
        out_specs=(P(), P(), P('row', None, None, 'col')),
        check_vma=False,
    )
```

```python
import jax
import jax.numpy as jnp
from jax import lax
from jax.experimental import pallas as pl
from jax.experimental.pallas import tpu as pltpu
from jax.sharding import PartitionSpec as P

STEPS = 4
F32 = jnp.float32
MIB = 2**20


(FAR_P, FAR_M, NEAR_P, NEAR_M, LO, HI, OWN_P, OWN_M, OWN_D, ALT_P, ALT_M, ALT_D, FWD_P, DP_O, DM_O, DP_A, DM_A,
 FWD_M, DF_O, DF_A) = range(20)
N_COPY, N_REDUCE = 20, 5


HALVES = (0, 1)
OTHERS = (1, 2, 3)
FAR_FIRST = (2, 1, 3)
CHIPS, CORES, ROWS = 4, 2, 8


def dot_hi(a, b):
    return lax.dot_general(a, b, (((1,), (0,)), ((), ())), precision=lax.Precision.HIGHEST, preferred_element_type=F32)


def hi_of(z):
    return lax.div(z, 2)


def lo_of(z):
    return lax.rem(lax.div(z + 1, 2), 2)


def remote(src, dst, send, recv, device):
    return pltpu.make_async_remote_copy(src_ref=src, dst_ref=dst, send_sem=send, recv_sem=recv, device_id=device,
                                        device_id_type=pl.DeviceIdType.MESH)


def signal(sem, device):
    pl.semaphore_signal(sem, inc=1, device_id=device, device_id_type=pl.DeviceIdType.MESH)


def block(start, n):
    return pl.ds(pl.multiple_of(start, n), n)


class Around:
    def __init__(self):
        self.row, self.col, self.mpo = (lax.axis_index(a) for a in ('row', 'col', 'mpo'))
        self.x, self.c = lax.div(self.row, CORES), lax.rem(self.row, CORES)
        self.hi, self.lo = hi_of(self.mpo), lo_of(self.mpo)
        (self.xp, self.x2, self.xm), (self.yp, self.y2, self.ym) = (
            [lax.rem(v + d, CHIPS) for d in OTHERS] for v in (self.x, self.col))
        self.other = 1 - self.c
        self.to_xp, self.to_xm = ({'row': v * CORES + self.c} for v in (self.xp, self.xm))
        self.to_core = {'row': self.x * CORES + self.other}
        self.to_yp, self.to_ym = {'col': self.yp}, {'col': self.ym}
        self.to_lo = {'mpo': self.mpo + 1 - CORES * lax.rem(self.mpo, CORES)}
        self.to_hi = {'mpo': CHIPS - 1 - self.mpo}

    def turn(self, **steps):
        size = {'row': ROWS, 'col': CHIPS, 'mpo': CHIPS}
        return {a: lax.rem(getattr(self, a) + d, size[a]) for a, d in steps.items()}


def got(ref, send, recv, device):
    remote(ref, ref, send, recv, device).wait_recv()


class Ring:
    def __init__(self, me, at, first, send, recv):
        x, c, o = me.x, me.c, me.other
        whole = [(at(me.xm, c), me.to_core), (at(me.xp, c), me.to_core)]
        halves = [at(me.x2, c, h) for h in HALVES]
        self.moves = [(first, at(x, c), d) for d in (me.to_xp, me.to_xm, me.to_core)]
        self.moves += [(r, r, d) for r, d in (
            (at(me.xm, c, 0), me.to_xp), (at(me.xp, c, 1), me.to_xm), *whole, *((h, me.to_core) for h in halves))]
        self.lands = [at(me.xm, c), at(me.xp, c), at(x, o), *halves, at(me.xm, o), at(me.xp, o),
                      *(at(me.x2, o, h) for h in HALVES)]
        self.send, self.recv, self.device = send, recv, me.to_core

    def copy(self, k):
        return remote(*self.moves[k][:2], self.send.at[k], self.recv.at[k], self.moves[k][-1])

    def start(self, *ks):
        for k in ks:
            self.copy(k).start()

    def sent(self):
        for k in range(len(self.moves)):
            self.copy(k).wait_send()

    def got(self, *ks):
        for k in ks:
            got(self.lands[k], self.send.at[k], self.recv.at[k], self.device)


(R_P, R_M, R_CORE, R_FWD_P, R_FWD_M, R_CORE_M, R_CORE_P, R_CORE_F0, R_CORE_F1) = range(9)


def lanczos(psi, left, right, w, out, ab, R, L, G, WG, U, W3, T1, T2, TP, PY, RF, RN, RZ, V, WS, ZB, AL, BE, BP, INV, OLD, ARS, AR1,
            AR2, l_s, l_r, ly_s, ly_r, psi_s, psi_r, rz_s, rz_r, rx_s, rx_r, rd_s, rd_r, w_s, w_r, local, send, recv,
            ar1_s, ar1_r, ar2_s, ar2_r, credit, z_s, z_r, o_s):
    me = Around()
    row, col, mpo, x, c, hi, lo = me.row, me.col, me.mpo, me.x, me.c, me.hi, me.lo
    n_s, nb, bh = G.shape
    aw, bw = nb // ROWS, CORES * bh
    ah = aw // 2
    n_r, alt, o, last = 2 * CHIPS, 1 - hi, me.other, n_s - 1
    here, me2 = me.to_core, col * CHIPS + mpo
    slices, tile = range(n_s), AL.shape[0]
    others = [(dc, dz) for dc in range(CHIPS) for dz in range(CHIPS) if dc or dz]
    peers = [me.turn(row=d) for d in range(1, ROWS)] + [me.turn(col=dc, mpo=dz) for dc, dz in others]
    plane = [(dr, dz) for dz in (*FAR_FIRST, 0) for dr in (4, 5, 2, 3, 6, 7, 1, 0)]

    bar = pltpu.get_barrier_semaphore()
    greeted = [me.turn(row=dr, mpo=dz) for dr, dz in plane[:-1]] + [me.turn(col=dc, mpo=dz) for dc, dz in others if dc]
    for peer in greeted:
        signal(bar, peer)
    pl.semaphore_wait(bar, len(greeted))

    wide = ROWS * ah
    q_even, q_odd = aw // CHIPS, ah // CHIPS

    def l_parts(z, y, first, n):
        def lanes(h):
            return pl.ds(pl.multiple_of(h * wide + first, ah), n)

        return (T2.at[z, block(lax.rem(y, 2) * q_even, q_even), lanes(lax.div(y, 2))],
                TP.at[z, block(y * q_odd, q_odd), lanes(0)], TP.at[z, :, lanes(1)])

    n_kinds = range(3)
    for kind in n_kinds:
        for dr, dz in plane:
            to = me.turn(row=dr, mpo=dz)
            cols = block(to['row'] * aw + hi_of(to['mpo']) * ah, ah)
            rows = (block(col * q_even, q_even), block(col * q_odd, q_odd), pl.ds(ah, ah))[kind]
            src = left.at[rows, min(kind, 1), cols]
            dst = l_parts(mpo, col, row * ah, ah)[kind]
            if dr or dz:
                remote(src, dst, l_s.at[kind], l_r.at[kind], to).start()
            else:
                pltpu.make_async_copy(src, dst, l_r.at[kind]).start()
        if kind == 1:
            def psi_at(t):
                def at(xx, core, h=None):
                    first = (xx * CORES + core) * aw
                    return G.at[t, block(first, aw) if h is None else block(first + h * ah, ah), :]
                return at

            def psi_src(t):
                return psi.at[:, t // 2, t % 2, block(lo * bh, bh)]

            psi_rings = [Ring(me, psi_at(t), psi_src(t), psi_s.at[t], psi_r.at[t]) for t in slices]
            for ring in psi_rings:
                ring.start(R_P, R_M, R_CORE)

    half, zc, xc = nb // 2, nb // CHIPS, nb // (2 * ROWS)

    def r_rows(q, rl):
        return block((q * 2 + rl) * bh, bh)

    def r_src(z, rl, first, n):
        return right.at[block(lo_of(z) * bh, bh), rl, block(first, n)]

    def x_cols(xx, core):
        return half + (xx * CORES + core) * xc

    def r_part(g):
        return (x_cols(x, c), xc) if g == 0 else (c * zc, zc)

    def r_copies(g):
        for dz in FAR_FIRST:
            to = me.turn(mpo=dz)
            for rl in HALVES:
                sems = rz_s.at[dz - 1, rl, g], rz_r.at[dz - 1, rl, g]
                yield remote(r_src(to['mpo'], rl, *r_part(g)), R.at[r_rows(CHIPS - dz, rl), block(*r_part(g))], *sems, to)

    def r_got(g):
        for dz in FAR_FIRST:
            for rl in HALVES:
                got(R.at[r_rows(CHIPS - dz, rl), block(*r_part(g))], rz_s.at[dz - 1, rl, g], rz_r.at[dz - 1, rl, g], here)

    def rx_at(xx, core, h=None):
        n = (n_r - 2) * bh
        rows = pl.ds(2 * bh, n) if h is None else pl.ds(2 * bh + h * n // 2, n // 2)
        return R.at[rows, block(x_cols(xx, core), xc)]

    rx = Ring(me, rx_at, rx_at(x, c), rx_s, rx_r)

    def rd_at(core):
        return R.at[pl.ds(2 * bh, (n_r - 2) * bh), block(core * zc, zc)]

    rd = remote(rd_at(c), rd_at(c), rd_s, rd_r, here)

    def w_copy(dz):
        return remote(w, WG.at[mpo], w_s.at[dz - 1], w_r.at[dz - 1], me.turn(mpo=dz))

    for dz in OTHERS:
        w_copy(dz).start()
    for g in HALVES:
        for part in r_copies(g):
            part.start()

    own = [(w, WG.at[mpo])] + [(psi_src(t), psi_at(t)(x, c)) for t in slices]
    own += [(r_src(mpo, rl, 0, nb), R.at[r_rows(0, rl), :]) for rl in HALVES]
    own = [pltpu.make_async_copy(src, dst, local.at[i]) for i, (src, dst) in enumerate(own)]
    for part in own:
        part.start()

    for ref in (V, BE, BP, INV, OLD):
        ref[...] = jnp.zeros_like(ref)

    def quarter(y, h=None):
        zs = slice(0, CHIPS) if h is None else slice(2 * h, 2 * h + 2)
        return [ref.at[zs] for ref in (T2.at[:, block(lax.rem(y, 2) * q_even, q_even), block(lax.div(y, 2) * wide, wide)],
                                       TP.at[:, block(y * q_odd, q_odd), pl.ds(0, wide)])]

    def ly(k):
        refs, to = ((quarter(col), me.to_yp), (quarter(col), me.to_ym), (quarter(me.ym, 0), me.to_yp),
                    (quarter(me.yp, 1), me.to_ym))[k]
        return [remote(ref, ref, ly_s.at[k, i], ly_r.at[k, i], to) for i, ref in enumerate(refs)]

    def ly_start(*ks):
        for k in ks:
            for part in ly(k):
                part.start()

    def ly_got(k):
        refs = (quarter(me.ym), quarter(me.yp), quarter(me.y2, 0), quarter(me.y2, 1))[k]
        for i, ref in enumerate(refs):
            got(ref, ly_s.at[k, i], ly_r.at[k, i], here)

    for kind, ref in enumerate(quarter(col)):
        got(ref, l_s.at[kind], l_r.at[kind], here)
    ly_start(0, 1)
    for k in HALVES:
        ly_got(k)
        ly_start(k + 2)
    for ring in psi_rings:
        ring.got(R_P)
        ring.start(R_FWD_P, R_CORE_M)
        ring.got(R_M)
        ring.start(R_FWD_M, R_CORE_P)
    r_got(0)
    rx.start(R_P, R_M, R_CORE)

    for dz in OTHERS:
        got(WG.at[lax.rem(mpo + CHIPS - dz, CHIPS)], w_s.at[dz - 1], w_r.at[dz - 1], here)
    own[0].wait()
    U[...] = jnp.concatenate([WG[z][:, :U.shape[1] // CHIPS] for z in range(CHIPS)], axis=1)
    lane, sub = (lax.broadcasted_iota(jnp.int32, (tile, U.shape[1]), i) for i in (1, 0))
    diagonal = jnp.where(lax.rem(lane, tile) == sub, 1.0, 0.0)
    for t in slices:
        for r in range(n_r):
            at = (t * n_r + r) * tile
            W3[at:at + tile] = U[pl.ds(t * n_r + lax.rem(r + 2 * mpo, n_r), 1), :] * diagonal

    for ring in psi_rings:
        ring.got(R_FWD_P)
        ring.start(R_CORE_F0)
        ring.got(R_FWD_M)
        ring.start(R_CORE_F1)
    got(TP.at[:, :, pl.ds(wide, wide)], l_s.at[2], l_r.at[2], here)
    for k in HALVES:
        ly_got(k + 2)
    for k in range(CHIPS):
        for part in ly(k):
            part.wait_send()

    @pl.loop(0, CHIPS)
    def _(z):
        for l, ref in enumerate((T2, TP)):
            for h in HALVES:
                for rr in range(ROWS):
                    first = h * wide + rr * ah
                    L[block((2 * z + l) * ah, ah), rr * aw + h * ah:rr * aw + (h + 1) * ah] = ref[z, :, first:first + ah].T

    for ref in (T2, TP):
        ref[...] = jnp.zeros_like(ref)
    for ring in psi_rings:
        ring.got(R_CORE, R_CORE_M, R_CORE_P, R_CORE_F0, R_CORE_F1)
    for part in own[1:1 + n_s]:
        part.wait()
    for ring in psi_rings:
        ring.sent()

    def r_round():
        rx.got(R_P)
        rx.start(R_FWD_P, R_CORE_M)
        rx.got(R_M)
        rx.start(R_FWD_M, R_CORE_P)

    def r_cores():
        r_got(1)
        rd.start()

    def r_far():
        rx.got(R_FWD_P)
        rx.start(R_CORE_F0)
        rx.got(R_FWD_M)
        rx.start(R_CORE_F1)

    def r_end():
        rx.got(R_CORE, R_CORE_M, R_CORE_P, R_CORE_F0, R_CORE_F1)
        got(rd_at(o), rd_s, rd_r, here)
        for part in own[1 + n_s:]:
            part.wait()
        rx.sent()
        for part in (*r_copies(0), *r_copies(1), *(w_copy(dz) for dz in OTHERS), rd):
            part.wait_send()
        for kind in n_kinds:
            for z, n in ((slice(0, CHIPS - 1), wide), (0, wide - ah)):
                ref = l_parts(z, col, 0, n)[kind]
                remote(ref, ref, l_s.at[kind], l_r.at[kind], here).wait_send()

    def rows_of(xx, cc, hh):
        return block((xx * CORES + cc) * aw + hh * ah, ah)

    own_rows = rows_of(x, c, hi)
    low, high = slice(0, bh), slice(bh, bw)

    def ends(k, t):
        def g_at(xx, cc, hh):
            return G.at[t, rows_of(xx, cc, hh), :]

        xp, xm, x2 = me.xp, me.xm, me.x2
        via = {
            HI: ((x, c, hi), (x, c, alt), me.to_hi),
            OWN_P: ((x, c, hi), (xm, c, hi), me.to_xp),
            OWN_M: ((x, c, hi), (xp, c, hi), me.to_xm),
            ALT_P: ((x, c, alt), (xm, c, alt), me.to_xp),
            ALT_M: ((x, c, alt), (xp, c, alt), me.to_xm),
            FWD_P: ((xm, c, hi), (x2, c, hi), me.to_xp),
            FWD_M: ((xp, c, alt), (x2, c, alt), me.to_xm),
        }
        for kind, xx, hh in ((OWN_D, x, hi), (ALT_D, x, alt), (DP_O, xp, hi), (DM_O, xm, hi), (DP_A, xp, alt),
                             (DM_A, xm, alt), (DF_O, x2, hi), (DF_A, x2, alt)):
            via[kind] = ((xx, c, hh), (xx, o, hh), me.to_core)
        if k in via:
            src, land, to = via[k]
            return g_at(*src), g_at(*src), g_at(*land), to
        far, plus, minus, own = (PY.at[t, i] for i in range(4))
        src, dst, to = {
            FAR_P: (far.at[:, low], RF.at[t, 0], me.to_yp),
            FAR_M: (far.at[:, high], RF.at[t, 1], me.to_ym),
            NEAR_P: (plus, RN.at[t, 0], me.to_yp),
            NEAR_M: (minus, RN.at[t, 1], me.to_ym),
            LO: (own.at[:, block((1 - lo) * bh, bh)], RZ.at[t], me.to_lo),
        }[k]
        return src, dst, dst, to

    def copy(k, t):
        src, dst, _, to = ends(k, t)
        return remote(src, dst, send.at[t, k], recv.at[t, k], to)

    def start(t, *kinds):
        for k in kinds:
            copy(k, t).start()

    def arrived(t, *kinds):
        for k in kinds:
            got(ends(k, t)[2], send.at[t, k], recv.at[t, k], here)

    def e1(t):
        start(t, FAR_P, FAR_M)

    def e2(t):
        arrived(t, FAR_P, FAR_M)
        PY[t, 1, :, low] += RF[t, 0]
        PY[t, 2, :, high] += RF[t, 1]
        start(t, NEAR_P, NEAR_M)

    def e3(t):
        arrived(t, NEAR_P, NEAR_M)
        PY[t, 3] += RN[t, 0] + RN[t, 1]
        start(t, LO)

    def e4(t):
        arrived(t, LO)
        G[t, own_rows, :] = (PY[t, 3, :, block(lo * bh, bh)] + RZ[t]) * INV[0:1, :]

    def g4(t):
        start(t, HI, OWN_P, OWN_M, OWN_D)

    def g5a(t):
        arrived(t, HI)
        start(t, ALT_P, ALT_M, ALT_D)

    def g5b(t):
        arrived(t, OWN_P)
        start(t, FWD_P, DM_O)
        arrived(t, OWN_M)
        start(t, DP_O)

    def g6a(t):
        arrived(t, ALT_M)
        start(t, FWD_M, DP_A)
        arrived(t, ALT_P)
        start(t, DM_A)

    def g6b(t):
        arrived(t, FWD_P)
        start(t, DF_O)

    def g7(t):
        arrived(t, FWD_M)
        start(t, DF_A)

    newest, oldest = STEPS % 2, 1 - STEPS % 2

    def z_copy(i, t, dz):
        return remote((RZ, WS)[i].at[t], ZB.at[i, t, dz - 1], z_s.at[i, t, dz - 1], z_r.at[i, t, dz - 1], me.turn(mpo=dz))

    def z_start(i, t):
        for dz in FAR_FIRST:
            z_copy(i, t, dz).start()

    def share(t):
        RZ[t] = G[t, own_rows, :] - BE[0:1, :] * V[oldest, t]
        z_start(0, t)

    def ar_pair(k, stage):
        slots, s_sem, r_sem = ((AR1, ar1_s, ar1_r), (AR2, ar2_s, ar2_r))[stage]
        n = len(peers) - len(others) if stage == 0 else len(others)
        ref = slots.at[k, 0:n]
        return remote(ref, ref, s_sem.at[k], r_sem.at[k], here)

    def ar_send(k, stage, part):
        slots, s_sem, r_sem, mine = ((AR1, ar1_s, ar1_r, row), (AR2, ar2_s, ar2_r, me2))[stage]
        ARS[k, stage] = part
        slots[k, mine] = part
        first = len(peers) - len(others)
        for peer in (peers[first:] if stage else peers[:first]):
            remote(ARS.at[k, stage], slots.at[k, mine], s_sem.at[k], r_sem.at[k], peer).start()

    def ar_sum(k, stage):
        ar_pair(k, stage).wait_recv()
        slots = (AR1, AR2)[stage]
        return sum((slots[k, i] for i in range(1, slots.shape[1])), slots[k, 0])

    def ar_end(k):
        tot = jnp.sum(ar_sum(k, 1))
        for stage in HALVES:
            ar_pair(k, stage).wait_send()
        return tot

    def fold(v):
        v = jnp.sum(v.reshape(ah // tile, tile, bh), axis=0)
        n = ARS.shape[-1]
        return sum((v[:, i:i + n] for i in range(n, bh, n)), v[:, :n])

    def a1(j):
        p = lax.rem(j, 2)
        parts = [fold(V[p, t] * G[t, own_rows, :]) for t in slices]
        ar_send(0, 0, sum(parts[1:], parts[0]))

    def a2():
        ar_send(0, 1, ar_sum(0, 0))

    def a3(j):
        p = lax.rem(j, 2)
        AL[...] = jnp.full(AL.shape, ar_end(0), F32)
        ab[0, j] = AL[:, :ab.shape[-1]]
        al, bp, parts = AL[0:1, :], BE[0:1, :], []
        for t in slices:
            w = (G[t, own_rows, :] - bp * V[1 - p, t]) - al * V[p, t]
            V[1 - p, t] = w
            parts.append(fold(w * w))
        ar_send(1, 0, sum(parts[1:], parts[0]))

    def b2():
        ar_send(1, 1, ar_sum(1, 0))

    def b3(j):
        p = lax.rem(j, 2)
        OLD[...] = INV[...]
        BP[...] = BE[...]
        BE[...] = jnp.sqrt(jnp.full(BE.shape, ar_end(1), F32))
        INV[...] = 1.0 / BE[...]
        for t in slices:
            V[1 - p, t] = V[1 - p, t] / BE[0:1, :]
        ab[1, j] = BE[:, :ab.shape[-1]]

    @pl.loop(0, STEPS)
    def _(j):
        first, later, more = j == 0, j > 0, j < STEPS - 1

        def t1_tick(s, xx, new=False):
            ks = block(xx * CORES * aw, CORES * aw)
            n = n_r * ah // 2
            for m in HALVES:
                ms = slice(m * n, (m + 1) * n)
                d = dot_hi(L[ms, ks], G[s, ks, :])
                if new:
                    T1[s, ms] = d
                else:
                    T1[s, ms] += d

        @pl.loop(0, n_s)
        def _(s):
            @pl.when(later)
            def _():
                for t in (2, 3):
                    @pl.when(s == t - 2)
                    def _():
                        e3(t)

                arrived(s, OWN_D, ALT_D)

            t1_tick(s, x, True)

            @pl.when(later)
            def _():
                g6b(s)

                @pl.when(s < last)
                def _():
                    g5a(s + 1)

                arrived(s, DM_O, DM_A)

            for i, event in enumerate((r_cores, r_round, r_far)):
                @pl.when(jnp.logical_and(first, s == i + 1))
                def _():
                    event()

            t1_tick(s, me.xm)

            @pl.when(later)
            def _():
                g7(s)

                @pl.when(s < last)
                def _():
                    g5b(s + 1)

                @pl.when(s < 2)
                def _():
                    e4(s + 2)
                    g4(s + 2)

                arrived(s, DP_O, DP_A)

            @pl.when(s == 2)
            def _():
                a2()

            t1_tick(s, me.xp)

            @pl.when(later)
            def _():
                @pl.when(s < last)
                def _():
                    g6a(s + 1)

                arrived(s, DF_O, DF_A)

            @pl.when(s == 1)
            def _():
                a1(j)

            t1_tick(s, me.x2)

        @pl.when(later)
        def _():
            @pl.loop(0, n_s)
            def _(t):
                for k in range(N_COPY):
                    copy(k, t).wait_send()

        @pl.when(more)
        def _():
            for i, peer in enumerate((me.to_hi, me.to_xp, me.to_xm, me.to_core)):
                signal(credit.at[i], peer)

        a3(j)

        @pl.when(jnp.logical_not(more))
        def _():
            for t in slices:
                WS[t] = V[newest, t]
                z_start(1, t)

        @pl.loop(0, ah // (4 * tile))
        def _(g):
            al, bp = AL[...] * INV[...], BE[...] * OLD[...]
            for u in range(4):
                at_row = pl.multiple_of((g * 4 + u) * tile, tile)
                mixed = dot_hi(W3[...], jnp.concatenate(
                    [T1[s, pl.ds((2 * z + l) * ah + at_row, tile), :]
                     for z in range(CHIPS) for s in slices for l in HALVES]))
                for t in slices:
                    for r in range(n_r):
                        i = (t * n_r + r) * tile
                        at = (t, pl.ds(at_row, tile), slice(r * bh, (r + 1) * bh))
                        now = T2[at]
                        T2[at] = mixed[i:i + tile] - al * now - bp * TP[at]
                        TP[at] = now

        @pl.when(first)
        def _():
            r_end()

        def y_tick(t, which, yy):
            PY[t, which] = dot_hi(T2[t], R[:, block(yy * bw, bw)])

        def far(t):
            y_tick(t, 0, me.y2)
            e1(t)

        far(0)
        b2()

        @pl.loop(0, n_s)
        def _(t):
            @pl.when(t < last)
            def _():
                far(t + 1)

            @pl.when(t == 1)
            def _():
                b3(j)

            @pl.when(t == 2)
            def _():
                e4(0)

                @pl.when(more)
                def _():
                    for i in range(credit.shape[0]):
                        pl.semaphore_wait(credit.at[i], 1)
                    g4(0)

                @pl.when(jnp.logical_not(more))
                def _():
                    share(0)

            @pl.when(jnp.logical_and(more, t == last))
            def _():
                g5a(0)

            y_tick(t, 1, me.yp)

            @pl.when(t == last)
            def _():
                e4(1)

                @pl.when(more)
                def _():
                    g5b(0)
                    g4(1)

                @pl.when(jnp.logical_not(more))
                def _():
                    share(1)

            y_tick(t, 2, me.ym)
            e2(t)

            for i in HALVES:
                @pl.when(t == i + 1)
                def _():
                    e3(i)

            @pl.when(jnp.logical_and(more, t == last))
            def _():
                g6a(0)

            y_tick(t, 3, col)

    for t in (2, last):
        e3(t)
    for t in (2, last):
        e4(t)
        share(t)
    a1(STEPS)
    a2()
    a3(STEPS)
    b2()
    for t in slices:
        for i in HALVES:
            for dz in OTHERS:
                got(ZB.at[i, t, dz - 1], z_s.at[i, t, dz - 1], z_r.at[i, t, dz - 1], here)
    b3(STEPS)

    def out_at(z):
        return block(lo_of(z) * aw + hi_of(z) * ah, ah)

    al, be = AL[0:1, :], BE[0:1, :]
    for t in slices:
        T1[t, out_at(mpo), :] = V[oldest, t]
        for dz in OTHERS:
            v = ZB[1, t, dz - 1] / BP[0:1, :]
            T1[t, out_at(lax.rem(mpo + CHIPS - dz, CHIPS)), :] = (ZB[0, t, dz - 1] - al * v) / be
        for h in HALVES:
            pltpu.make_async_copy(T1.at[t, h * aw:(h + 1) * aw, :], out.at[:, t // 2, t % 2, h * bh:(h + 1) * bh],
                                  o_s.at[t, h]).start()
    for t in slices:
        for k in range(N_REDUCE):
            copy(k, t).wait_send()
        for i in HALVES:
            for dz in OTHERS:
                z_copy(i, t, dz).wait_send()
        for h in HALVES:
            pltpu.make_async_copy(T1.at[t, h * aw:(h + 1) * aw, :], out.at[:, t // 2, t % 2, h * bh:(h + 1) * bh],
                                  o_s.at[t, h]).wait()


def solution(mesh):
    dma = pltpu.SemaphoreType.DMA
    anywhere, vmem = (pl.BlockSpec(memory_space=m) for m in (pl.ANY, pltpu.VMEM))

    def shape(*dims):
        return jax.ShapeDtypeStruct(dims, F32)

    def keep(*dims, dtype=F32):
        return pltpu.VMEM(dims, dtype)

    def local_fn(psi_blk, left_blk, right_blk, mpo_blk):
        aw, bw, nb = psi_blk.shape[0], psi_blk.shape[-1], right_blk.shape[-1]
        ah, bh, n_l, n_s = aw // 2, bw // 2, 2 * CHIPS, CHIPS
        tile, lanes = 8, min(128, bh)
        w = mpo_blk.reshape(2, n_l, n_s, n_s).transpose(3, 1, 2, 0).reshape(n_s * n_l, n_l)
        w = jnp.pad(jnp.repeat(w, tile, axis=1), ((0, 0), (0, n_l * tile)))
        two, nine, far = dma((2,)), dma((9,)), dma((3,))
        v_next, ab = pl.pallas_call(
            lanczos,
            out_shape=(shape(*psi_blk.shape), shape(2, STEPS + 1, tile, lanes)),
            in_specs=[anywhere] * 4,
            out_specs=[anywhere, vmem],
            scratch_shapes=[
                keep(n_l * bh, nb), keep(n_l * ah, nb), keep(n_s, nb, bh), keep(CHIPS, *w.shape), keep(n_s * n_l, 256),
                keep(256, 256), keep(n_s, n_l * ah, bh), keep(n_s, ah, n_l * bh), keep(n_s, ah, n_l * bh),
                keep(n_s, 4, ah, bw), keep(n_s, 2, ah, bh), keep(n_s, 2, ah, bw), keep(n_s, ah, bh),
                keep(2, n_s, ah, bh), keep(n_s, ah, bh), keep(2, n_s, 3, ah, bh), *[keep(tile, bh)] * 5,
                keep(2, 2, tile, lanes), keep(2, ROWS, tile, lanes), keep(2, CHIPS * CHIPS, tile, lanes),
                far, far, dma((4, 2)), dma((4, 2)), dma((n_s, 9)), dma((n_s, 9)), dma((3, 2, 2)), dma((3, 2, 2)),
                nine, nine, dma, dma, far, far, dma((7,)),
                dma((n_s, N_COPY)), dma((n_s, N_COPY)), two, two, two, two,
                pltpu.SemaphoreType.REGULAR((4,)), dma((2, n_s, 3)), dma((2, n_s, 3)),
                dma((n_s, 2)),
            ],
            compiler_params=pltpu.CompilerParams(collective_id=0, has_side_effects=True, vmem_limit_bytes=62 * MIB),
            name='lanczos',
        )(psi_blk, left_blk, right_blk, w)
        return ab[0, 1:, 0, 0], ab[1, 1:, 0, 0], v_next

    return jax.shard_map(
        local_fn,
        mesh=mesh,
        in_specs=(P('row', None, None, 'col'), P('row', 'mpo', None), P('col', 'mpo', None),
                  P('mpo', None, None, None, None, None)),
        out_specs=(P(), P(), P('row', None, None, 'col')),
        check_vma=False,
    )
```

```python
import jax
import jax.numpy as jnp
from jax import lax
from jax.experimental import pallas as pl
from jax.experimental.pallas import tpu as pltpu
from jax.sharding import PartitionSpec as P

STEPS = 4
F32 = jnp.float32
MIB = 2**20


(FAR_P, FAR_M, NEAR_P, NEAR_M, LO, HI, OWN_P, OWN_M, OWN_D, ALT_P, ALT_M, ALT_D, FWD_P, DP_O, DM_O, DP_A, DM_A,
 FWD_M, DF_O, DF_A) = range(20)
N_COPY, N_REDUCE = 20, 5


HALVES = (0, 1)
OTHERS = (1, 2, 3)
FAR_FIRST = (2, 1, 3)
CHIPS, CORES, ROWS = 4, 2, 8


def dot_hi(a, b):
    return lax.dot_general(a, b, (((1,), (0,)), ((), ())), precision=lax.Precision.HIGHEST, preferred_element_type=F32)


def hi_of(z):
    return lax.div(z, 2)


def lo_of(z):
    return lax.rem(lax.div(z + 1, 2), 2)


def remote(src, dst, send, recv, device):
    return pltpu.make_async_remote_copy(src_ref=src, dst_ref=dst, send_sem=send, recv_sem=recv, device_id=device,
                                        device_id_type=pl.DeviceIdType.MESH)


def signal(sem, device):
    pl.semaphore_signal(sem, inc=1, device_id=device, device_id_type=pl.DeviceIdType.MESH)


def block(start, n):
    return pl.ds(pl.multiple_of(start, n), n)


class Around:
    def __init__(self):
        self.row, self.col, self.mpo = (lax.axis_index(a) for a in ('row', 'col', 'mpo'))
        self.x, self.c = lax.div(self.row, CORES), lax.rem(self.row, CORES)
        self.hi, self.lo = hi_of(self.mpo), lo_of(self.mpo)
        (self.xp, self.x2, self.xm), (self.yp, self.y2, self.ym) = (
            [lax.rem(v + d, CHIPS) for d in OTHERS] for v in (self.x, self.col))
        self.other = 1 - self.c
        self.to_xp, self.to_xm = ({'row': v * CORES + self.c} for v in (self.xp, self.xm))
        self.to_core = {'row': self.x * CORES + self.other}
        self.to_yp, self.to_ym = {'col': self.yp}, {'col': self.ym}
        self.to_lo = {'mpo': self.mpo + 1 - CORES * lax.rem(self.mpo, CORES)}
        self.to_hi = {'mpo': CHIPS - 1 - self.mpo}

    def turn(self, **steps):
        size = {'row': ROWS, 'col': CHIPS, 'mpo': CHIPS}
        return {a: lax.rem(getattr(self, a) + d, size[a]) for a, d in steps.items()}


def got(ref, send, recv, device):
    remote(ref, ref, send, recv, device).wait_recv()


class Ring:
    def __init__(self, me, at, first, send, recv):
        x, c, o = me.x, me.c, me.other
        whole = [(at(me.xm, c), me.to_core), (at(me.xp, c), me.to_core)]
        halves = [at(me.x2, c, h) for h in HALVES]
        self.moves = [(first, at(x, c), d) for d in (me.to_xp, me.to_xm, me.to_core)]
        self.moves += [(r, r, d) for r, d in (
            (at(me.xm, c, 0), me.to_xp), (at(me.xp, c, 1), me.to_xm), *whole, *((h, me.to_core) for h in halves))]
        self.lands = [at(me.xm, c), at(me.xp, c), at(x, o), *halves, at(me.xm, o), at(me.xp, o),
                      *(at(me.x2, o, h) for h in HALVES)]
        self.send, self.recv, self.device = send, recv, me.to_core

    def copy(self, k):
        return remote(*self.moves[k][:2], self.send.at[k], self.recv.at[k], self.moves[k][-1])

    def start(self, *ks):
        for k in ks:
            self.copy(k).start()

    def sent(self):
        for k in range(len(self.moves)):
            self.copy(k).wait_send()

    def got(self, *ks):
        for k in ks:
            got(self.lands[k], self.send.at[k], self.recv.at[k], self.device)


(R_P, R_M, R_CORE, R_FWD_P, R_FWD_M, R_CORE_M, R_CORE_P, R_CORE_F0, R_CORE_F1) = range(9)


def lanczos(psi, left, right, w, out, ab, R, L, G, WG, U, W3, T1, T2, TP, PY, RF, RN, RZ, V, WS, ZB, AL, BE, BP, INV, OLD, ARS, AR1,
            AR2, l_s, l_r, ly_s, ly_r, psi_s, psi_r, rz_s, rz_r, rx_s, rx_r, rd_s, rd_r, w_s, w_r, local, send, recv,
            ar1_s, ar1_r, ar2_s, ar2_r, credit, z_s, z_r, o_s):
    me = Around()
    row, col, mpo, x, c, hi, lo = me.row, me.col, me.mpo, me.x, me.c, me.hi, me.lo
    n_s, nb, bh = G.shape
    aw, bw = nb // ROWS, CORES * bh
    ah = aw // 2
    n_r, alt, o, last = 2 * CHIPS, 1 - hi, me.other, n_s - 1
    here, me2 = me.to_core, col * CHIPS + mpo
    slices, tile = range(n_s), AL.shape[0]
    others = [(dc, dz) for dc in range(CHIPS) for dz in range(CHIPS) if dc or dz]
    peers = [me.turn(row=d) for d in range(1, ROWS)] + [me.turn(col=dc, mpo=dz) for dc, dz in others]
    plane = [(dr, dz) for dz in (*FAR_FIRST, 0) for dr in (4, 5, 2, 3, 6, 7, 1, 0)]

    bar = pltpu.get_barrier_semaphore()
    greeted = [me.turn(row=dr, mpo=dz) for dr, dz in plane[:-1]] + [me.turn(col=dc, mpo=dz) for dc, dz in others if dc]
    for peer in greeted:
        signal(bar, peer)
    pl.semaphore_wait(bar, len(greeted))

    wide = ROWS * ah
    quart, few = aw // CHIPS, ah // 2
    near = lax.div(col, 2)

    def l_part(ref, z, first, n):
        return ref.at[z, block(lax.rem(col, 2) * quart, quart), pl.ds(pl.multiple_of(near * wide + first, ah), n)]

    landing = (T2, TP)
    for l, ref in enumerate(landing):
        for dr, dz in plane:
            to = me.turn(row=dr, mpo=dz)
            src = left.at[block(col * quart, quart), l, block(to['row'] * aw + hi_of(to['mpo']) * ah, ah)]
            dst = l_part(ref, mpo, row * ah, ah)
            if dr or dz:
                remote(src, dst, l_s.at[l], l_r.at[l], to).start()
            else:
                pltpu.make_async_copy(src, dst, l_r.at[l]).start()

    def psi_at(t, h):
        def at(xx, core, k=None):
            base = h * wide + (xx * CORES + core) * ah
            return G.at[t, block(base, ah) if k is None else block(base + k * few, few), :]
        return at

    def psi_src(t, h):
        return psi.at[h * ah:(h + 1) * ah, t // 2, t % 2, block(lo * bh, bh)]

    psi_parts = [(t, h) for t in slices for h in HALVES]
    psi_rings = [Ring(me, psi_at(*part), psi_src(*part), psi_s.at[i], psi_r.at[i]) for i, part in enumerate(psi_parts)]
    for ring in psi_rings:
        ring.start(R_P, R_M, R_CORE)

    half, zc, xc = nb // 2, nb // CHIPS, nb // (2 * ROWS)

    def r_rows(q, rl):
        return block((q * 2 + rl) * bh, bh)

    def r_src(z, rl, first, n):
        return right.at[block(lo_of(z) * bh, bh), rl, block(first, n)]

    def x_cols(xx, core):
        return half + (xx * CORES + core) * xc

    def r_part(g):
        return (x_cols(x, c), xc) if g == 0 else (c * zc, zc)

    def r_copies(g):
        for dz in FAR_FIRST:
            to = me.turn(mpo=dz)
            for rl in HALVES:
                sems = rz_s.at[dz - 1, rl, g], rz_r.at[dz - 1, rl, g]
                yield remote(r_src(to['mpo'], rl, *r_part(g)), R.at[r_rows(CHIPS - dz, rl), block(*r_part(g))], *sems, to)

    def r_got(g):
        for dz in FAR_FIRST:
            for rl in HALVES:
                got(R.at[r_rows(CHIPS - dz, rl), block(*r_part(g))], rz_s.at[dz - 1, rl, g], rz_r.at[dz - 1, rl, g], here)

    def rx_at(xx, core, h=None):
        n = (n_r - 2) * bh
        rows = pl.ds(2 * bh, n) if h is None else pl.ds(2 * bh + h * n // 2, n // 2)
        return R.at[rows, block(x_cols(xx, core), xc)]

    rx = Ring(me, rx_at, rx_at(x, c), rx_s, rx_r)

    def rd_at(core):
        return R.at[pl.ds(2 * bh, (n_r - 2) * bh), block(core * zc, zc)]

    rd = remote(rd_at(c), rd_at(c), rd_s, rd_r, here)

    def w_copy(dz):
        return remote(w, WG.at[mpo], w_s.at[dz - 1], w_r.at[dz - 1], me.turn(mpo=dz))

    for dz in OTHERS:
        w_copy(dz).start()
    for g in HALVES:
        for part in r_copies(g):
            part.start()

    own = [(w, WG.at[mpo])] + [(psi_src(*part), psi_at(*part)(x, c)) for part in psi_parts]
    own += [(r_src(mpo, rl, 0, nb), R.at[r_rows(0, rl), :]) for rl in HALVES]
    own = [pltpu.make_async_copy(src, dst, local.at[i]) for i, (src, dst) in enumerate(own)]
    for part in own:
        part.start()

    for ref in (V, BE, BP, INV, OLD):
        ref[...] = jnp.zeros_like(ref)

    def quarter(y, h=None):
        zs = slice(0, CHIPS) if h is None else slice(2 * h, 2 * h + 2)
        rows, lanes = block(lax.rem(y, 2) * quart, quart), block(lax.div(y, 2) * wide, wide)
        return [ref.at[zs, rows, lanes] for ref in landing]

    def ly(k):
        refs, to = ((quarter(col), me.to_yp), (quarter(col), me.to_ym), (quarter(me.ym, 0), me.to_yp),
                    (quarter(me.yp, 1), me.to_ym))[k]
        return [remote(ref, ref, ly_s.at[k, i], ly_r.at[k, i], to) for i, ref in enumerate(refs)]

    def ly_got(l, *ks):
        for k in ks:
            ref = (quarter(me.ym), quarter(me.yp), quarter(me.y2, 0), quarter(me.y2, 1))[k][l]
            got(ref, ly_s.at[k, l], ly_r.at[k, l], here)

    def ly_on(l):
        for k in HALVES:
            ly_got(l, k)
            ly(k + 2)[l].start()

    for l in HALVES:
        got(quarter(col)[l], l_s.at[l], l_r.at[l], here)
        for k in HALVES:
            ly(k)[l].start()
    ly_on(0)
    for ring in psi_rings:
        ring.got(R_P)
        ring.start(R_FWD_P, R_CORE_M)
        ring.got(R_M)
        ring.start(R_FWD_M, R_CORE_P)
    r_got(0)
    rx.start(R_P, R_M, R_CORE)

    for dz in OTHERS:
        got(WG.at[lax.rem(mpo + CHIPS - dz, CHIPS)], w_s.at[dz - 1], w_r.at[dz - 1], here)
    own[0].wait()
    U[...] = jnp.concatenate([WG[z][:, :U.shape[1] // CHIPS] for z in range(CHIPS)], axis=1)
    lane, sub = (lax.broadcasted_iota(jnp.int32, (tile, U.shape[1]), i) for i in (1, 0))
    diagonal = jnp.where(lax.rem(lane, tile) == sub, 1.0, 0.0)
    for t in slices:
        for r in range(n_r):
            at = (t * n_r + r) * tile
            W3[at:at + tile] = U[pl.ds(t * n_r + lax.rem(r + 2 * mpo, n_r), 1), :] * diagonal

    ly_on(1)
    for ring in psi_rings:
        ring.got(R_FWD_P)
        ring.start(R_CORE_F0)
        ring.got(R_FWD_M)
        ring.start(R_CORE_F1)

    def turn_over(h):
        @pl.loop(0, CHIPS)
        def _(z):
            for l, ref in enumerate(landing):
                for rr in range(ROWS):
                    lanes = block(h * wide + rr * ah, ah)
                    L[block((2 * z + l) * ah, ah), lanes] = ref[z, :, lanes].T

    turn_over(near)
    for ring in psi_rings:
        ring.got(R_CORE, R_CORE_M, R_CORE_P, R_CORE_F0, R_CORE_F1)
    for part in own[1:1 + len(psi_parts)]:
        part.wait()
    for ring in psi_rings:
        ring.sent()

    def r_round():
        rx.got(R_P)
        rx.start(R_FWD_P, R_CORE_M)
        rx.got(R_M)
        rx.start(R_FWD_M, R_CORE_P)

    def r_cores():
        r_got(1)
        rd.start()

    def r_far():
        rx.got(R_FWD_P)
        rx.start(R_CORE_F0)
        rx.got(R_FWD_M)
        rx.start(R_CORE_F1)

    def r_end():
        rx.got(R_CORE, R_CORE_M, R_CORE_P, R_CORE_F0, R_CORE_F1)
        got(rd_at(o), rd_s, rd_r, here)
        for part in own[1 + len(psi_parts):]:
            part.wait()
        rx.sent()
        for part in (*r_copies(0), *r_copies(1), *(w_copy(dz) for dz in OTHERS), rd):
            part.wait_send()
        for l, ref in enumerate(landing):
            for z, n in ((slice(0, CHIPS - 1), wide), (0, wide - ah)):
                part = l_part(ref, z, 0, n)
                remote(part, part, l_s.at[l], l_r.at[l], here).wait_send()

    def rows_of(xx, cc, hh):
        return block(hh * wide + (xx * CORES + cc) * ah, ah)

    own_rows = rows_of(x, c, hi)
    low, high = slice(0, bh), slice(bh, bw)

    def ends(k, t):
        def g_at(xx, cc, hh):
            return G.at[t, rows_of(xx, cc, hh), :]

        xp, xm, x2 = me.xp, me.xm, me.x2
        via = {
            HI: ((x, c, hi), (x, c, alt), me.to_hi),
            OWN_P: ((x, c, hi), (xm, c, hi), me.to_xp),
            OWN_M: ((x, c, hi), (xp, c, hi), me.to_xm),
            ALT_P: ((x, c, alt), (xm, c, alt), me.to_xp),
            ALT_M: ((x, c, alt), (xp, c, alt), me.to_xm),
            FWD_P: ((xm, c, hi), (x2, c, hi), me.to_xp),
            FWD_M: ((xp, c, alt), (x2, c, alt), me.to_xm),
        }
        for kind, xx, hh in ((OWN_D, x, hi), (ALT_D, x, alt), (DP_O, xp, hi), (DM_O, xm, hi), (DP_A, xp, alt),
                             (DM_A, xm, alt), (DF_O, x2, hi), (DF_A, x2, alt)):
            via[kind] = ((xx, c, hh), (xx, o, hh), me.to_core)
        if k in via:
            src, land, to = via[k]
            return g_at(*src), g_at(*src), g_at(*land), to
        far, plus, minus, own = (PY.at[t, i] for i in range(4))
        src, dst, to = {
            FAR_P: (far.at[:, low], RF.at[t, 0], me.to_yp),
            FAR_M: (far.at[:, high], RF.at[t, 1], me.to_ym),
            NEAR_P: (plus, RN.at[t, 0], me.to_yp),
            NEAR_M: (minus, RN.at[t, 1], me.to_ym),
            LO: (own.at[:, block((1 - lo) * bh, bh)], RZ.at[t], me.to_lo),
        }[k]
        return src, dst, dst, to

    def copy(k, t):
        src, dst, _, to = ends(k, t)
        return remote(src, dst, send.at[t, k], recv.at[t, k], to)

    def start(t, *kinds):
        for k in kinds:
            copy(k, t).start()

    def arrived(t, *kinds):
        for k in kinds:
            got(ends(k, t)[2], send.at[t, k], recv.at[t, k], here)

    def e1(t):
        start(t, FAR_P, FAR_M)

    def e2(t):
        arrived(t, FAR_P, FAR_M)
        PY[t, 1, :, low] += RF[t, 0]
        PY[t, 2, :, high] += RF[t, 1]
        start(t, NEAR_P, NEAR_M)

    def e3(t):
        arrived(t, NEAR_P, NEAR_M)
        PY[t, 3] += RN[t, 0] + RN[t, 1]
        start(t, LO)

    def e4(t):
        arrived(t, LO)
        G[t, own_rows, :] = (PY[t, 3, :, block(lo * bh, bh)] + RZ[t]) * INV[0:1, :]

    def g4(t):
        start(t, HI, OWN_P, OWN_M, OWN_D)

    def g5a(t):
        arrived(t, HI)
        start(t, ALT_P, ALT_M, ALT_D)

    def g5b(t):
        arrived(t, OWN_P)
        start(t, FWD_P, DM_O)
        arrived(t, OWN_M)
        start(t, DP_O)

    def g6a(t):
        arrived(t, ALT_M)
        start(t, FWD_M, DP_A)
        arrived(t, ALT_P)
        start(t, DM_A)

    def g6b(t):
        arrived(t, FWD_P)
        start(t, DF_O)

    def g7(t):
        arrived(t, FWD_M)
        start(t, DF_A)

    newest, oldest = STEPS % 2, 1 - STEPS % 2

    def z_copy(i, t, dz):
        return remote((RZ, WS)[i].at[t], ZB.at[i, t, dz - 1], z_s.at[i, t, dz - 1], z_r.at[i, t, dz - 1], me.turn(mpo=dz))

    def z_start(i, t):
        for dz in FAR_FIRST:
            z_copy(i, t, dz).start()

    def share(t):
        RZ[t] = G[t, own_rows, :] - BE[0:1, :] * V[oldest, t]
        z_start(0, t)

    def ar_pair(k, stage):
        slots, s_sem, r_sem = ((AR1, ar1_s, ar1_r), (AR2, ar2_s, ar2_r))[stage]
        n = len(peers) - len(others) if stage == 0 else len(others)
        ref = slots.at[k, 0:n]
        return remote(ref, ref, s_sem.at[k], r_sem.at[k], here)

    def ar_send(k, stage, part):
        slots, s_sem, r_sem, mine = ((AR1, ar1_s, ar1_r, row), (AR2, ar2_s, ar2_r, me2))[stage]
        ARS[k, stage] = part
        slots[k, mine] = part
        first = len(peers) - len(others)
        for peer in (peers[first:] if stage else peers[:first]):
            remote(ARS.at[k, stage], slots.at[k, mine], s_sem.at[k], r_sem.at[k], peer).start()

    def ar_sum(k, stage):
        ar_pair(k, stage).wait_recv()
        slots = (AR1, AR2)[stage]
        return sum((slots[k, i] for i in range(1, slots.shape[1])), slots[k, 0])

    def ar_end(k):
        tot = jnp.sum(ar_sum(k, 1))
        for stage in HALVES:
            ar_pair(k, stage).wait_send()
        return tot

    def fold(v):
        v = jnp.sum(v.reshape(ah // tile, tile, bh), axis=0)
        n = ARS.shape[-1]
        return sum((v[:, i:i + n] for i in range(n, bh, n)), v[:, :n])

    def a1(j):
        p = lax.rem(j, 2)
        parts = [fold(V[p, t] * G[t, own_rows, :]) for t in slices]
        ar_send(0, 0, sum(parts[1:], parts[0]))

    def a2():
        ar_send(0, 1, ar_sum(0, 0))

    def a3(j):
        p = lax.rem(j, 2)
        AL[...] = jnp.full(AL.shape, ar_end(0), F32)
        ab[0, j] = AL[:, :ab.shape[-1]]
        al, bp, parts = AL[0:1, :], BE[0:1, :], []
        for t in slices:
            w = (G[t, own_rows, :] - bp * V[1 - p, t]) - al * V[p, t]
            V[1 - p, t] = w
            parts.append(fold(w * w))
        ar_send(1, 0, sum(parts[1:], parts[0]))

    def b2():
        ar_send(1, 1, ar_sum(1, 0))

    def b3(j):
        p = lax.rem(j, 2)
        OLD[...] = INV[...]
        BP[...] = BE[...]
        BE[...] = jnp.sqrt(jnp.full(BE.shape, ar_end(1), F32))
        INV[...] = 1.0 / BE[...]
        for t in slices:
            V[1 - p, t] = V[1 - p, t] / BE[0:1, :]
        ab[1, j] = BE[:, :ab.shape[-1]]

    def t1_half(h, new, events):
        ks = block(h * wide, wide)

        @pl.loop(0, n_s)
        def _(s):
            for m in HALVES:
                ms = slice(m * n_r * ah // 2, (m + 1) * n_r * ah // 2)
                d = dot_hi(L[ms, ks], G[s, ks, :])
                if new:
                    T1[s, ms] = d
                else:
                    T1[s, ms] += d

            for when, event in events:
                @pl.when(s == when)
                def _():
                    event()

    AL[...] = jnp.zeros_like(AL)
    ab[0, 0] = jnp.zeros(ab.shape[2:], F32)
    parts = []
    for t in slices:
        V[1, t] = G[t, own_rows, :]
        parts.append(fold(V[1, t] * V[1, t]))
    ar_send(1, 0, sum(parts[1:], parts[0]))
    t1_half(near, True, ((2, r_round),))
    for l in HALVES:
        ly_got(l, 2, 3)
    turn_over(1 - near)
    t1_half(1 - near, False, ((0, r_cores), (1, r_far)))
    for k in range(CHIPS):
        for part in ly(k):
            part.wait_send()
    for ref in landing:
        ref[...] = jnp.zeros_like(ref)

    @pl.loop(0, STEPS)
    def _(j):
        first, later, more = j == 0, j > 0, j < STEPS - 1

        def t1_tick(s, xx, new=False):
            for m in HALVES:
                ms = slice(m * n_r * ah // 2, (m + 1) * n_r * ah // 2)
                ks = [block(h * wide + xx * CORES * ah, CORES * ah) for h in HALVES]
                d = dot_hi(L[ms, ks[0]], G[s, ks[0], :]) + dot_hi(L[ms, ks[1]], G[s, ks[1], :])
                if new:
                    T1[s, ms] = d
                else:
                    T1[s, ms] += d

        def t1_slice(s):
            for t in (2, 3):
                @pl.when(s == t - 2)
                def _():
                    e3(t)

            arrived(s, OWN_D, ALT_D)
            t1_tick(s, x, True)
            g6b(s)

            @pl.when(s < last)
            def _():
                g5a(s + 1)

            arrived(s, DM_O, DM_A)
            t1_tick(s, me.xm)
            g7(s)

            @pl.when(s < last)
            def _():
                g5b(s + 1)

            @pl.when(s < 2)
            def _():
                e4(s + 2)
                g4(s + 2)

            arrived(s, DP_O, DP_A)

            @pl.when(s == 2)
            def _():
                a2()

            t1_tick(s, me.xp)

            @pl.when(s < last)
            def _():
                g6a(s + 1)

            arrived(s, DF_O, DF_A)

            @pl.when(s == 1)
            def _():
                a1(j)

            t1_tick(s, me.x2)

        @pl.when(later)
        def _():
            pl.loop(0, n_s)(t1_slice)

        @pl.when(later)
        def _():
            @pl.loop(0, n_s)
            def _(t):
                for k in range(N_COPY):
                    copy(k, t).wait_send()

        @pl.when(more)
        def _():
            for i, peer in enumerate((me.to_hi, me.to_xp, me.to_xm, me.to_core)):
                signal(credit.at[i], peer)

        @pl.when(later)
        def _():
            a3(j)

        @pl.when(jnp.logical_not(more))
        def _():
            for t in slices:
                WS[t] = V[newest, t]
                z_start(1, t)

        @pl.loop(0, ah // (4 * tile))
        def _(g):
            al, bp = AL[...] * INV[...], BE[...] * OLD[...]
            for u in range(4):
                at_row = pl.multiple_of((g * 4 + u) * tile, tile)
                mixed = dot_hi(W3[...], jnp.concatenate(
                    [T1[s, pl.ds((2 * z + l) * ah + at_row, tile), :]
                     for z in range(CHIPS) for s in slices for l in HALVES]))
                for t in slices:
                    for r in range(n_r):
                        i = (t * n_r + r) * tile
                        at = (t, pl.ds(at_row, tile), slice(r * bh, (r + 1) * bh))
                        now = T2[at]
                        T2[at] = mixed[i:i + tile] - al * now - bp * TP[at]
                        TP[at] = now

        @pl.when(first)
        def _():
            r_end()

        def y_tick(t, which, yy):
            PY[t, which] = dot_hi(T2[t], R[:, block(yy * bw, bw)])

        def far(t):
            y_tick(t, 0, me.y2)
            e1(t)

        far(0)
        b2()

        @pl.loop(0, n_s)
        def _(t):
            @pl.when(t < last)
            def _():
                far(t + 1)

            @pl.when(t == 1)
            def _():
                b3(j)

            @pl.when(t == 2)
            def _():
                e4(0)

                @pl.when(more)
                def _():
                    for i in range(credit.shape[0]):
                        pl.semaphore_wait(credit.at[i], 1)
                    g4(0)

                @pl.when(jnp.logical_not(more))
                def _():
                    share(0)

            @pl.when(jnp.logical_and(more, t == last))
            def _():
                g5a(0)

            y_tick(t, 1, me.yp)

            @pl.when(t == last)
            def _():
                e4(1)

                @pl.when(more)
                def _():
                    g5b(0)
                    g4(1)

                @pl.when(jnp.logical_not(more))
                def _():
                    share(1)

            y_tick(t, 2, me.ym)
            e2(t)

            for i in HALVES:
                @pl.when(t == i + 1)
                def _():
                    e3(i)

            @pl.when(jnp.logical_and(more, t == last))
            def _():
                g6a(0)

            y_tick(t, 3, col)

    for t in (2, last):
        e3(t)
    for t in (2, last):
        e4(t)
        share(t)
    a1(STEPS)
    a2()
    a3(STEPS)
    b2()
    for t in slices:
        for i in HALVES:
            for dz in OTHERS:
                got(ZB.at[i, t, dz - 1], z_s.at[i, t, dz - 1], z_r.at[i, t, dz - 1], here)
    b3(STEPS)

    def out_at(z):
        return block(lo_of(z) * aw + hi_of(z) * ah, ah)

    al, be = AL[0:1, :], BE[0:1, :]
    for t in slices:
        T1[t, out_at(mpo), :] = V[oldest, t]
        for dz in OTHERS:
            v = ZB[1, t, dz - 1] / BP[0:1, :]
            T1[t, out_at(lax.rem(mpo + CHIPS - dz, CHIPS)), :] = (ZB[0, t, dz - 1] - al * v) / be
        for h in HALVES:
            pltpu.make_async_copy(T1.at[t, h * aw:(h + 1) * aw, :], out.at[:, t // 2, t % 2, h * bh:(h + 1) * bh],
                                  o_s.at[t, h]).start()
    for t in slices:
        for k in range(N_REDUCE):
            copy(k, t).wait_send()
        for i in HALVES:
            for dz in OTHERS:
                z_copy(i, t, dz).wait_send()
        for h in HALVES:
            pltpu.make_async_copy(T1.at[t, h * aw:(h + 1) * aw, :], out.at[:, t // 2, t % 2, h * bh:(h + 1) * bh],
                                  o_s.at[t, h]).wait()


def solution(mesh):
    dma = pltpu.SemaphoreType.DMA
    anywhere, vmem = (pl.BlockSpec(memory_space=m) for m in (pl.ANY, pltpu.VMEM))

    def shape(*dims):
        return jax.ShapeDtypeStruct(dims, F32)

    def keep(*dims, dtype=F32):
        return pltpu.VMEM(dims, dtype)

    def local_fn(psi_blk, left_blk, right_blk, mpo_blk):
        aw, bw, nb = psi_blk.shape[0], psi_blk.shape[-1], right_blk.shape[-1]
        ah, bh, n_l, n_s = aw // 2, bw // 2, 2 * CHIPS, CHIPS
        tile, lanes = 8, min(128, bh)
        w = mpo_blk.reshape(2, n_l, n_s, n_s).transpose(3, 1, 2, 0).reshape(n_s * n_l, n_l)
        w = jnp.pad(jnp.repeat(w, tile, axis=1), ((0, 0), (0, n_l * tile)))
        two, nine, far = dma((2,)), dma((9,)), dma((3,))
        v_next, ab = pl.pallas_call(
            lanczos,
            out_shape=(shape(*psi_blk.shape), shape(2, STEPS + 1, tile, lanes)),
            in_specs=[anywhere] * 4,
            out_specs=[anywhere, vmem],
            scratch_shapes=[
                keep(n_l * bh, nb), keep(n_l * ah, nb), keep(n_s, nb, bh), keep(CHIPS, *w.shape), keep(n_s * n_l, 256),
                keep(256, 256), keep(n_s, n_l * ah, bh), keep(n_s, ah, n_l * bh), keep(n_s, ah, n_l * bh),
                keep(n_s, 4, ah, bw), keep(n_s, 2, ah, bh), keep(n_s, 2, ah, bw), keep(n_s, ah, bh),
                keep(2, n_s, ah, bh), keep(n_s, ah, bh), keep(2, n_s, 3, ah, bh), *[keep(tile, bh)] * 5,
                keep(2, 2, tile, lanes), keep(2, ROWS, tile, lanes), keep(2, CHIPS * CHIPS, tile, lanes),
                two, two, dma((4, 2)), dma((4, 2)), dma((n_l, 9)), dma((n_l, 9)), dma((3, 2, 2)), dma((3, 2, 2)),
                nine, nine, dma, dma, far, far, dma((11,)),
                dma((n_s, N_COPY)), dma((n_s, N_COPY)), two, two, two, two,
                pltpu.SemaphoreType.REGULAR((4,)), dma((2, n_s, 3)), dma((2, n_s, 3)),
                dma((n_s, 2)),
            ],
            compiler_params=pltpu.CompilerParams(collective_id=0, has_side_effects=True, vmem_limit_bytes=62 * MIB),
            name='lanczos',
        )(psi_blk, left_blk, right_blk, w)
        return ab[0, 1:, 0, 0], ab[1, 1:, 0, 0], v_next

    return jax.shard_map(
        local_fn,
        mesh=mesh,
        in_specs=(P('row', None, None, 'col'), P('row', 'mpo', None), P('col', 'mpo', None),
                  P('mpo', None, None, None, None, None)),
        out_specs=(P(), P(), P('row', None, None, 'col')),
        check_vma=False,
    )
```

```python
import jax
import jax.numpy as jnp
from jax import lax
from jax.experimental import pallas as pl
from jax.experimental.pallas import tpu as pltpu
from jax.sharding import PartitionSpec as P

STEPS = 4
F32 = jnp.float32
MIB = 2**20


(FAR_P, FAR_M, NEAR_P, NEAR_M, LO, HI, OWN_P, OWN_M, OWN_D, ALT_P, ALT_M, ALT_D, FWD_P, DP_O, DM_O, DP_A, DM_A,
 FWD_M, DF_O, DF_A) = range(20)
N_COPY, N_REDUCE = 20, 5


HALVES = (0, 1)
OTHERS = (1, 2, 3)
FAR_FIRST = (2, 1, 3)
CHIPS, CORES, ROWS = 4, 2, 8


def dot_hi(a, b):
    return lax.dot_general(a, b, (((1,), (0,)), ((), ())), precision=lax.Precision.HIGHEST, preferred_element_type=F32)


def hi_of(z):
    return lax.div(z, 2)


def lo_of(z):
    return lax.rem(lax.div(z + 1, 2), 2)


def remote(src, dst, send, recv, device):
    return pltpu.make_async_remote_copy(src_ref=src, dst_ref=dst, send_sem=send, recv_sem=recv, device_id=device,
                                        device_id_type=pl.DeviceIdType.MESH)


def signal(sem, device):
    pl.semaphore_signal(sem, inc=1, device_id=device, device_id_type=pl.DeviceIdType.MESH)


def block(start, n):
    return pl.ds(pl.multiple_of(start, n), n)


class Around:
    def __init__(self):
        self.row, self.col, self.mpo = (lax.axis_index(a) for a in ('row', 'col', 'mpo'))
        self.x, self.c = lax.div(self.row, CORES), lax.rem(self.row, CORES)
        self.hi, self.lo = hi_of(self.mpo), lo_of(self.mpo)
        (self.xp, self.x2, self.xm), (self.yp, self.y2, self.ym) = (
            [lax.rem(v + d, CHIPS) for d in OTHERS] for v in (self.x, self.col))
        self.other = 1 - self.c
        self.to_xp, self.to_xm = ({'row': v * CORES + self.c} for v in (self.xp, self.xm))
        self.to_core = {'row': self.x * CORES + self.other}
        self.to_yp, self.to_ym = {'col': self.yp}, {'col': self.ym}
        self.to_lo = {'mpo': self.mpo + 1 - CORES * lax.rem(self.mpo, CORES)}
        self.to_hi = {'mpo': CHIPS - 1 - self.mpo}

    def turn(self, **steps):
        size = {'row': ROWS, 'col': CHIPS, 'mpo': CHIPS}
        return {a: lax.rem(getattr(self, a) + d, size[a]) for a, d in steps.items()}


def got(ref, send, recv, device):
    remote(ref, ref, send, recv, device).wait_recv()


class Ring:
    def __init__(self, me, at, first, send, recv):
        x, c, o = me.x, me.c, me.other
        whole = [(at(me.xm, c), me.to_core), (at(me.xp, c), me.to_core)]
        halves = [at(me.x2, c, h) for h in HALVES]
        self.moves = [(first, at(x, c), d) for d in (me.to_xp, me.to_xm, me.to_core)]
        self.moves += [(r, r, d) for r, d in (
            (at(me.xm, c, 0), me.to_xp), (at(me.xp, c, 1), me.to_xm), *whole, *((h, me.to_core) for h in halves))]
        self.lands = [at(me.xm, c), at(me.xp, c), at(x, o), *halves, at(me.xm, o), at(me.xp, o),
                      *(at(me.x2, o, h) for h in HALVES)]
        self.send, self.recv, self.device = send, recv, me.to_core

    def copy(self, k):
        return remote(*self.moves[k][:2], self.send.at[k], self.recv.at[k], self.moves[k][-1])

    def start(self, *ks):
        for k in ks:
            self.copy(k).start()

    def sent(self):
        for k in range(len(self.moves)):
            self.copy(k).wait_send()

    def got(self, *ks):
        for k in ks:
            got(self.lands[k], self.send.at[k], self.recv.at[k], self.device)


(R_P, R_M, R_CORE, R_FWD_P, R_FWD_M, R_CORE_M, R_CORE_P, R_CORE_F0, R_CORE_F1) = range(9)


def lanczos(psi, left, right, w, out, ab, R, L, G, WG, U, W3, T1, T2, TP, PY, RF, RN, RZ, V, WS, ZB, AL, BE, BP, INV, OLD, ARS, AR1,
            AR2, l_s, l_r, ly_s, ly_r, psi_s, psi_r, rz_s, rz_r, rx_s, rx_r, rd_s, rd_r, w_s, w_r, local, send, recv,
            ar1_s, ar1_r, ar2_s, ar2_r, credit, z_s, z_r, o_s):
    me = Around()
    row, col, mpo, x, c, hi, lo = me.row, me.col, me.mpo, me.x, me.c, me.hi, me.lo
    n_s, nb, bh = G.shape
    aw, bw = nb // ROWS, CORES * bh
    ah = aw // 2
    n_r, alt, o, last = 2 * CHIPS, 1 - hi, me.other, n_s - 1
    here, me2 = me.to_core, col * CHIPS + mpo
    slices, tile = range(n_s), AL.shape[0]
    others = [(dc, dz) for dc in range(CHIPS) for dz in range(CHIPS) if dc or dz]
    peers = [me.turn(row=d) for d in range(1, ROWS)] + [me.turn(col=dc, mpo=dz) for dc, dz in others]
    plane = [(dr, dz) for dz in (*FAR_FIRST, 0) for dr in (4, 5, 2, 3, 6, 7, 1, 0)]

    bar = pltpu.get_barrier_semaphore()
    greeted = [me.turn(row=dr, mpo=dz) for dr, dz in plane[:-1]] + [me.turn(col=dc, mpo=dz) for dc, dz in others if dc]
    for peer in greeted:
        signal(bar, peer)
    pl.semaphore_wait(bar, len(greeted))

    wide = ROWS * ah
    quart, few = aw // CHIPS, ah // 2
    near = lax.div(col, 2)

    def l_part(ref, z, first, n):
        return ref.at[z, block(lax.rem(col, 2) * quart, quart), pl.ds(pl.multiple_of(near * wide + first, ah), n)]

    landing = (T2, TP)
    for l, ref in enumerate(landing):
        for dr, dz in plane:
            to = me.turn(row=dr, mpo=dz)
            src = left.at[block(col * quart, quart), l, block(to['row'] * aw + hi_of(to['mpo']) * ah, ah)]
            dst = l_part(ref, mpo, row * ah, ah)
            if dr or dz:
                remote(src, dst, l_s.at[l], l_r.at[l], to).start()
            else:
                pltpu.make_async_copy(src, dst, l_r.at[l]).start()

    def psi_at(t, h):
        def at(xx, core, k=None):
            base = h * wide + (xx * CORES + core) * ah
            return G.at[t, block(base, ah) if k is None else block(base + k * few, few), :]
        return at

    def psi_src(t, h):
        return psi.at[h * ah:(h + 1) * ah, t // 2, t % 2, block(lo * bh, bh)]

    psi_parts = [(t, h) for t in slices for h in HALVES]
    psi_rings = [Ring(me, psi_at(*part), psi_src(*part), psi_s.at[i], psi_r.at[i]) for i, part in enumerate(psi_parts)]
    for ring in psi_rings:
        ring.start(R_P, R_M, R_CORE)

    half, zc, xc = nb // 2, nb // CHIPS, nb // (2 * ROWS)

    def r_rows(q, rl):
        return block((q * 2 + rl) * bh, bh)

    def r_src(z, rl, first, n):
        return right.at[block(lo_of(z) * bh, bh), rl, block(first, n)]

    def x_cols(xx, core):
        return half + (xx * CORES + core) * xc

    def r_part(g):
        return (x_cols(x, c), xc) if g == 0 else (c * zc, zc)

    def r_copies(g):
        for dz in FAR_FIRST:
            to = me.turn(mpo=dz)
            for rl in HALVES:
                sems = rz_s.at[dz - 1, rl, g], rz_r.at[dz - 1, rl, g]
                yield remote(r_src(to['mpo'], rl, *r_part(g)), R.at[r_rows(CHIPS - dz, rl), block(*r_part(g))], *sems, to)

    def r_got(g):
        for dz in FAR_FIRST:
            for rl in HALVES:
                got(R.at[r_rows(CHIPS - dz, rl), block(*r_part(g))], rz_s.at[dz - 1, rl, g], rz_r.at[dz - 1, rl, g], here)

    def rx_at(xx, core, h=None):
        n = (n_r - 2) * bh
        rows = pl.ds(2 * bh, n) if h is None else pl.ds(2 * bh + h * n // 2, n // 2)
        return R.at[rows, block(x_cols(xx, core), xc)]

    rx = Ring(me, rx_at, rx_at(x, c), rx_s, rx_r)

    def rd_at(core):
        return R.at[pl.ds(2 * bh, (n_r - 2) * bh), block(core * zc, zc)]

    rd = remote(rd_at(c), rd_at(c), rd_s, rd_r, here)

    def w_copy(dz):
        return remote(w, WG.at[mpo], w_s.at[dz - 1], w_r.at[dz - 1], me.turn(mpo=dz))

    for dz in OTHERS:
        w_copy(dz).start()
    for g in HALVES:
        for part in r_copies(g):
            part.start()

    own = [(w, WG.at[mpo])] + [(psi_src(*part), psi_at(*part)(x, c)) for part in psi_parts]
    own += [(r_src(mpo, rl, 0, nb), R.at[r_rows(0, rl), :]) for rl in HALVES]
    own = [pltpu.make_async_copy(src, dst, local.at[i]) for i, (src, dst) in enumerate(own)]
    for part in own:
        part.start()

    for ref in (V, BE, BP, INV, OLD):
        ref[...] = jnp.zeros_like(ref)

    def quarter(y, h=None):
        zs = slice(0, CHIPS) if h is None else slice(2 * h, 2 * h + 2)
        rows, lanes = block(lax.rem(y, 2) * quart, quart), block(lax.div(y, 2) * wide, wide)
        return [ref.at[zs, rows, lanes] for ref in landing]

    def ly(k):
        refs, to = ((quarter(col), me.to_yp), (quarter(col), me.to_ym), (quarter(me.ym, 0), me.to_yp),
                    (quarter(me.yp, 1), me.to_ym))[k]
        return [remote(ref, ref, ly_s.at[k, i], ly_r.at[k, i], to) for i, ref in enumerate(refs)]

    def ly_got(l, *ks):
        for k in ks:
            ref = (quarter(me.ym), quarter(me.yp), quarter(me.y2, 0), quarter(me.y2, 1))[k][l]
            got(ref, ly_s.at[k, l], ly_r.at[k, l], here)

    def ly_on(l):
        for k in HALVES:
            ly_got(l, k)
            ly(k + 2)[l].start()

    for l in HALVES:
        got(quarter(col)[l], l_s.at[l], l_r.at[l], here)
        for k in HALVES:
            ly(k)[l].start()
    ly_on(0)
    for ring in psi_rings:
        ring.got(R_P)
        ring.start(R_FWD_P, R_CORE_M)
        ring.got(R_M)
        ring.start(R_FWD_M, R_CORE_P)
    r_got(0)
    rx.start(R_P, R_M, R_CORE)

    for dz in OTHERS:
        got(WG.at[lax.rem(mpo + CHIPS - dz, CHIPS)], w_s.at[dz - 1], w_r.at[dz - 1], here)
    own[0].wait()
    U[...] = jnp.concatenate([WG[z][:, :U.shape[1] // CHIPS] for z in range(CHIPS)], axis=1)
    lane, sub = (lax.broadcasted_iota(jnp.int32, (tile, U.shape[1]), i) for i in (1, 0))
    diagonal = jnp.where(lax.rem(lane, tile) == sub, 1.0, 0.0)
    for t in slices:
        for r in range(n_r):
            at = (t * n_r + r) * tile
            W3[at:at + tile] = U[pl.ds(t * n_r + lax.rem(r + 2 * mpo, n_r), 1), :] * diagonal

    ly_on(1)
    for ring in psi_rings:
        ring.got(R_FWD_P)
        ring.start(R_CORE_F0)
        ring.got(R_FWD_M)
        ring.start(R_CORE_F1)

    def turn_over(h, which=HALVES):
        @pl.loop(0, CHIPS)
        def _(z):
            for l in which:
                for rr in range(ROWS):
                    lanes = block(h * wide + rr * ah, ah)
                    L[block((l * CHIPS + z) * ah, ah), lanes] = landing[l][z, :, lanes].T

    turn_over(near)
    for ring in psi_rings:
        ring.got(R_CORE, R_CORE_M, R_CORE_P, R_CORE_F0, R_CORE_F1)
    for part in own[1:1 + len(psi_parts)]:
        part.wait()
    for ring in psi_rings:
        ring.sent()

    def r_round():
        rx.got(R_P)
        rx.start(R_FWD_P, R_CORE_M)
        rx.got(R_M)
        rx.start(R_FWD_M, R_CORE_P)

    def r_cores():
        r_got(1)
        rd.start()

    def r_far():
        rx.got(R_FWD_P)
        rx.start(R_CORE_F0)
        rx.got(R_FWD_M)
        rx.start(R_CORE_F1)

    def r_end():
        rx.got(R_CORE, R_CORE_M, R_CORE_P, R_CORE_F0, R_CORE_F1)
        got(rd_at(o), rd_s, rd_r, here)
        for part in own[1 + len(psi_parts):]:
            part.wait()
        rx.sent()
        for part in (*r_copies(0), *r_copies(1), *(w_copy(dz) for dz in OTHERS), rd):
            part.wait_send()
        for l, ref in enumerate(landing):
            for z, n in ((slice(0, CHIPS - 1), wide), (0, wide - ah)):
                part = l_part(ref, z, 0, n)
                remote(part, part, l_s.at[l], l_r.at[l], here).wait_send()

    def rows_of(xx, cc, hh):
        return block(hh * wide + (xx * CORES + cc) * ah, ah)

    own_rows = rows_of(x, c, hi)
    low, high = slice(0, bh), slice(bh, bw)

    def ends(k, t):
        def g_at(xx, cc, hh):
            return G.at[t, rows_of(xx, cc, hh), :]

        xp, xm, x2 = me.xp, me.xm, me.x2
        via = {
            HI: ((x, c, hi), (x, c, alt), me.to_hi),
            OWN_P: ((x, c, hi), (xm, c, hi), me.to_xp),
            OWN_M: ((x, c, hi), (xp, c, hi), me.to_xm),
            ALT_P: ((x, c, alt), (xm, c, alt), me.to_xp),
            ALT_M: ((x, c, alt), (xp, c, alt), me.to_xm),
            FWD_P: ((xm, c, hi), (x2, c, hi), me.to_xp),
            FWD_M: ((xp, c, alt), (x2, c, alt), me.to_xm),
        }
        for kind, xx, hh in ((OWN_D, x, hi), (ALT_D, x, alt), (DP_O, xp, hi), (DM_O, xm, hi), (DP_A, xp, alt),
                             (DM_A, xm, alt), (DF_O, x2, hi), (DF_A, x2, alt)):
            via[kind] = ((xx, c, hh), (xx, o, hh), me.to_core)
        if k in via:
            src, land, to = via[k]
            return g_at(*src), g_at(*src), g_at(*land), to
        far, plus, minus, own = (PY.at[t, i] for i in range(4))
        src, dst, to = {
            FAR_P: (far.at[:, low], RF.at[t, 0], me.to_yp),
            FAR_M: (far.at[:, high], RF.at[t, 1], me.to_ym),
            NEAR_P: (plus, RN.at[t, 0], me.to_yp),
            NEAR_M: (minus, RN.at[t, 1], me.to_ym),
            LO: (own.at[:, block((1 - lo) * bh, bh)], RZ.at[t], me.to_lo),
        }[k]
        return src, dst, dst, to

    def copy(k, t):
        src, dst, _, to = ends(k, t)
        return remote(src, dst, send.at[t, k], recv.at[t, k], to)

    def start(t, *kinds):
        for k in kinds:
            copy(k, t).start()

    def arrived(t, *kinds):
        for k in kinds:
            got(ends(k, t)[2], send.at[t, k], recv.at[t, k], here)

    def e1(t):
        start(t, FAR_P, FAR_M)

    def e2(t):
        arrived(t, FAR_P, FAR_M)
        PY[t, 1, :, low] += RF[t, 0]
        PY[t, 2, :, high] += RF[t, 1]
        start(t, NEAR_P, NEAR_M)

    def e3(t):
        arrived(t, NEAR_P, NEAR_M)
        PY[t, 3] += RN[t, 0] + RN[t, 1]
        start(t, LO)

    def e4(t):
        arrived(t, LO)
        G[t, own_rows, :] = (PY[t, 3, :, block(lo * bh, bh)] + RZ[t]) * INV[0:1, :]

    def g4(t):
        start(t, HI, OWN_P, OWN_M, OWN_D)

    def g5a(t):
        arrived(t, HI)
        start(t, ALT_P, ALT_M, ALT_D)

    def g5b(t):
        arrived(t, OWN_P)
        start(t, FWD_P, DM_O)
        arrived(t, OWN_M)
        start(t, DP_O)

    def g6a(t):
        arrived(t, ALT_M)
        start(t, FWD_M, DP_A)
        arrived(t, ALT_P)
        start(t, DM_A)

    def g6b(t):
        arrived(t, FWD_P)
        start(t, DF_O)

    def g7(t):
        arrived(t, FWD_M)
        start(t, DF_A)

    newest, oldest = STEPS % 2, 1 - STEPS % 2

    def z_copy(i, t, dz):
        return remote((RZ, WS)[i].at[t], ZB.at[i, t, dz - 1], z_s.at[i, t, dz - 1], z_r.at[i, t, dz - 1], me.turn(mpo=dz))

    def z_start(i, t):
        for dz in FAR_FIRST:
            z_copy(i, t, dz).start()

    def share(t):
        RZ[t] = G[t, own_rows, :] - BE[0:1, :] * V[oldest, t]
        z_start(0, t)

    def ar_pair(k, stage):
        slots, s_sem, r_sem = ((AR1, ar1_s, ar1_r), (AR2, ar2_s, ar2_r))[stage]
        n = len(peers) - len(others) if stage == 0 else len(others)
        ref = slots.at[k, 0:n]
        return remote(ref, ref, s_sem.at[k], r_sem.at[k], here)

    def ar_send(k, stage, part):
        slots, s_sem, r_sem, mine = ((AR1, ar1_s, ar1_r, row), (AR2, ar2_s, ar2_r, me2))[stage]
        ARS[k, stage] = part
        slots[k, mine] = part
        first = len(peers) - len(others)
        for peer in (peers[first:] if stage else peers[:first]):
            remote(ARS.at[k, stage], slots.at[k, mine], s_sem.at[k], r_sem.at[k], peer).start()

    def ar_sum(k, stage):
        ar_pair(k, stage).wait_recv()
        slots = (AR1, AR2)[stage]
        return sum((slots[k, i] for i in range(1, slots.shape[1])), slots[k, 0])

    def ar_end(k):
        tot = jnp.sum(ar_sum(k, 1))
        for stage in HALVES:
            ar_pair(k, stage).wait_send()
        return tot

    def fold(v):
        v = jnp.sum(v.reshape(ah // tile, tile, bh), axis=0)
        n = ARS.shape[-1]
        return sum((v[:, i:i + n] for i in range(n, bh, n)), v[:, :n])

    def a1(j):
        p = lax.rem(j, 2)
        parts = [fold(V[p, t] * G[t, own_rows, :]) for t in slices]
        ar_send(0, 0, sum(parts[1:], parts[0]))

    def a2():
        ar_send(0, 1, ar_sum(0, 0))

    def a3(j):
        p = lax.rem(j, 2)
        AL[...] = jnp.full(AL.shape, ar_end(0), F32)
        ab[0, j] = AL[:, :ab.shape[-1]]
        al, bp, parts = AL[0:1, :], BE[0:1, :], []
        for t in slices:
            w = (G[t, own_rows, :] - bp * V[1 - p, t]) - al * V[p, t]
            V[1 - p, t] = w
            parts.append(fold(w * w))
        ar_send(1, 0, sum(parts[1:], parts[0]))

    def b2():
        ar_send(1, 1, ar_sum(1, 0))

    def b3(j):
        p = lax.rem(j, 2)
        OLD[...] = INV[...]
        BP[...] = BE[...]
        BE[...] = jnp.sqrt(jnp.full(BE.shape, ar_end(1), F32))
        INV[...] = 1.0 / BE[...]
        for t in slices:
            V[1 - p, t] = V[1 - p, t] / BE[0:1, :]
        ab[1, j] = BE[:, :ab.shape[-1]]

    def t1_half(h, new, events, which=HALVES):
        ks = block(h * wide, wide)

        @pl.loop(0, n_s)
        def _(s):
            for m in which:
                ms = slice(m * n_r * ah // 2, (m + 1) * n_r * ah // 2)
                d = dot_hi(L[ms, ks], G[s, ks, :])
                if new:
                    T1[s, ms] = d
                else:
                    T1[s, ms] += d

            for when, event in events:
                @pl.when(s == when)
                def _():
                    event()

    AL[...] = jnp.zeros_like(AL)
    ab[0, 0] = jnp.zeros(ab.shape[2:], F32)
    parts = []
    for t in slices:
        V[1, t] = G[t, own_rows, :]
        parts.append(fold(V[1, t] * V[1, t]))
    ar_send(1, 0, sum(parts[1:], parts[0]))
    t1_half(near, True, ((2, r_round),))
    for l, events in enumerate(((), ((0, r_cores), (1, r_far)))):
        ly_got(l, 2, 3)
        turn_over(1 - near, (l,))
        t1_half(1 - near, False, events, (l,))
    for k in range(CHIPS):
        for part in ly(k):
            part.wait_send()
    for ref in landing:
        ref[...] = jnp.zeros_like(ref)

    @pl.loop(0, STEPS)
    def _(j):
        first, later, more = j == 0, j > 0, j < STEPS - 1

        def t1_tick(s, xx, new=False):
            for m in HALVES:
                ms = slice(m * n_r * ah // 2, (m + 1) * n_r * ah // 2)
                ks = [block(h * wide + xx * CORES * ah, CORES * ah) for h in HALVES]
                d = dot_hi(L[ms, ks[0]], G[s, ks[0], :]) + dot_hi(L[ms, ks[1]], G[s, ks[1], :])
                if new:
                    T1[s, ms] = d
                else:
                    T1[s, ms] += d

        def t1_slice(s):
            for t in (2, 3):
                @pl.when(s == t - 2)
                def _():
                    e3(t)

            arrived(s, OWN_D, ALT_D)
            t1_tick(s, x, True)
            g6b(s)

            @pl.when(s < last)
            def _():
                g5a(s + 1)

            arrived(s, DM_O, DM_A)
            t1_tick(s, me.xm)
            g7(s)

            @pl.when(s < last)
            def _():
                g5b(s + 1)

            @pl.when(s < 2)
            def _():
                e4(s + 2)
                g4(s + 2)

            arrived(s, DP_O, DP_A)

            @pl.when(s == 2)
            def _():
                a2()

            t1_tick(s, me.xp)

            @pl.when(s < last)
            def _():
                g6a(s + 1)

            arrived(s, DF_O, DF_A)

            @pl.when(s == 1)
            def _():
                a1(j)

            t1_tick(s, me.x2)

        @pl.when(later)
        def _():
            pl.loop(0, n_s)(t1_slice)

        @pl.when(later)
        def _():
            @pl.loop(0, n_s)
            def _(t):
                for k in range(N_COPY):
                    copy(k, t).wait_send()

        @pl.when(more)
        def _():
            for i, peer in enumerate((me.to_hi, me.to_xp, me.to_xm, me.to_core)):
                signal(credit.at[i], peer)

        @pl.when(later)
        def _():
            a3(j)

        @pl.when(jnp.logical_not(more))
        def _():
            for t in slices:
                WS[t] = V[newest, t]
                z_start(1, t)

        @pl.loop(0, ah // (4 * tile))
        def _(g):
            al, bp = AL[...] * INV[...], BE[...] * OLD[...]
            for u in range(4):
                at_row = pl.multiple_of((g * 4 + u) * tile, tile)
                mixed = dot_hi(W3[...], jnp.concatenate(
                    [T1[s, pl.ds((l * CHIPS + z) * ah + at_row, tile), :]
                     for z in range(CHIPS) for s in slices for l in HALVES]))
                for t in slices:
                    for r in range(n_r):
                        i = (t * n_r + r) * tile
                        at = (t, pl.ds(at_row, tile), slice(r * bh, (r + 1) * bh))
                        now = T2[at]
                        T2[at] = mixed[i:i + tile] - al * now - bp * TP[at]
                        TP[at] = now

        @pl.when(first)
        def _():
            r_end()

        def y_tick(t, which, yy):
            PY[t, which] = dot_hi(T2[t], R[:, block(yy * bw, bw)])

        def far(t):
            y_tick(t, 0, me.y2)
            e1(t)

        far(0)
        b2()

        @pl.loop(0, n_s)
        def _(t):
            @pl.when(t < last)
            def _():
                far(t + 1)

            @pl.when(t == 1)
            def _():
                b3(j)

            @pl.when(t == 2)
            def _():
                e4(0)

                @pl.when(more)
                def _():
                    for i in range(credit.shape[0]):
                        pl.semaphore_wait(credit.at[i], 1)
                    g4(0)

                @pl.when(jnp.logical_not(more))
                def _():
                    share(0)

            @pl.when(jnp.logical_and(more, t == last))
            def _():
                g5a(0)

            y_tick(t, 1, me.yp)

            @pl.when(t == last)
            def _():
                e4(1)

                @pl.when(more)
                def _():
                    g5b(0)
                    g4(1)

                @pl.when(jnp.logical_not(more))
                def _():
                    share(1)

            y_tick(t, 2, me.ym)
            e2(t)

            for i in HALVES:
                @pl.when(t == i + 1)
                def _():
                    e3(i)

            @pl.when(jnp.logical_and(more, t == last))
            def _():
                g6a(0)

            y_tick(t, 3, col)

    for t in (2, last):
        e3(t)
    for t in (2, last):
        e4(t)
        share(t)
    a1(STEPS)
    a2()
    a3(STEPS)
    b2()
    for t in slices:
        for i in HALVES:
            for dz in OTHERS:
                got(ZB.at[i, t, dz - 1], z_s.at[i, t, dz - 1], z_r.at[i, t, dz - 1], here)
    b3(STEPS)

    def out_at(z):
        return block(lo_of(z) * aw + hi_of(z) * ah, ah)

    al, be = AL[0:1, :], BE[0:1, :]
    for t in slices:
        T1[t, out_at(mpo), :] = V[oldest, t]
        for dz in OTHERS:
            v = ZB[1, t, dz - 1] / BP[0:1, :]
            T1[t, out_at(lax.rem(mpo + CHIPS - dz, CHIPS)), :] = (ZB[0, t, dz - 1] - al * v) / be
        for h in HALVES:
            pltpu.make_async_copy(T1.at[t, h * aw:(h + 1) * aw, :], out.at[:, t // 2, t % 2, h * bh:(h + 1) * bh],
                                  o_s.at[t, h]).start()
    for t in slices:
        for k in range(N_REDUCE):
            copy(k, t).wait_send()
        for i in HALVES:
            for dz in OTHERS:
                z_copy(i, t, dz).wait_send()
        for h in HALVES:
            pltpu.make_async_copy(T1.at[t, h * aw:(h + 1) * aw, :], out.at[:, t // 2, t % 2, h * bh:(h + 1) * bh],
                                  o_s.at[t, h]).wait()


def solution(mesh):
    dma = pltpu.SemaphoreType.DMA
    anywhere, vmem = (pl.BlockSpec(memory_space=m) for m in (pl.ANY, pltpu.VMEM))

    def shape(*dims):
        return jax.ShapeDtypeStruct(dims, F32)

    def keep(*dims, dtype=F32):
        return pltpu.VMEM(dims, dtype)

    def local_fn(psi_blk, left_blk, right_blk, mpo_blk):
        aw, bw, nb = psi_blk.shape[0], psi_blk.shape[-1], right_blk.shape[-1]
        ah, bh, n_l, n_s = aw // 2, bw // 2, 2 * CHIPS, CHIPS
        tile, lanes = 8, min(128, bh)
        w = mpo_blk.reshape(2, n_l, n_s, n_s).transpose(3, 1, 2, 0).reshape(n_s * n_l, n_l)
        w = jnp.pad(jnp.repeat(w, tile, axis=1), ((0, 0), (0, n_l * tile)))
        two, nine, far = dma((2,)), dma((9,)), dma((3,))
        v_next, ab = pl.pallas_call(
            lanczos,
            out_shape=(shape(*psi_blk.shape), shape(2, STEPS + 1, tile, lanes)),
            in_specs=[anywhere] * 4,
            out_specs=[anywhere, vmem],
            scratch_shapes=[
                keep(n_l * bh, nb), keep(n_l * ah, nb), keep(n_s, nb, bh), keep(CHIPS, *w.shape), keep(n_s * n_l, 256),
                keep(256, 256), keep(n_s, n_l * ah, bh), keep(n_s, ah, n_l * bh), keep(n_s, ah, n_l * bh),
                keep(n_s, 4, ah, bw), keep(n_s, 2, ah, bh), keep(n_s, 2, ah, bw), keep(n_s, ah, bh),
                keep(2, n_s, ah, bh), keep(n_s, ah, bh), keep(2, n_s, 3, ah, bh), *[keep(tile, bh)] * 5,
                keep(2, 2, tile, lanes), keep(2, ROWS, tile, lanes), keep(2, CHIPS * CHIPS, tile, lanes),
                two, two, dma((4, 2)), dma((4, 2)), dma((n_l, 9)), dma((n_l, 9)), dma((3, 2, 2)), dma((3, 2, 2)),
                nine, nine, dma, dma, far, far, dma((11,)),
                dma((n_s, N_COPY)), dma((n_s, N_COPY)), two, two, two, two,
                pltpu.SemaphoreType.REGULAR((4,)), dma((2, n_s, 3)), dma((2, n_s, 3)),
                dma((n_s, 2)),
            ],
            compiler_params=pltpu.CompilerParams(collective_id=0, has_side_effects=True, vmem_limit_bytes=62 * MIB),
            name='lanczos',
        )(psi_blk, left_blk, right_blk, w)
        return ab[0, 1:, 0, 0], ab[1, 1:, 0, 0], v_next

    return jax.shard_map(
        local_fn,
        mesh=mesh,
        in_specs=(P('row', None, None, 'col'), P('row', 'mpo', None), P('col', 'mpo', None),
                  P('mpo', None, None, None, None, None)),
        out_specs=(P(), P(), P('row', None, None, 'col')),
        check_vma=False,
    )
```
